16 devices in a mesh: model: 2 (over z), data: 8 (over y, x, core).
Axes of the slice: x: 2, y: 2, z: 2, core: 2. Of those that a mesh axis runs over, the one named last changes fastest.
Arguments:
- dec_in: bfloat16 [128, 384, 512], P('data')
- enc_out: bfloat16 [128, 192, 512], P('data')
- grad_out: bfloat16 [128, 384, 512], P('data')
- rel_bias: bfloat16 [32, 6], P(None, 'model')
- self_q: bfloat16 [512, 384], P('data', 'model')
- self_k: bfloat16 [512, 384], P('data', 'model')
- self_v: bfloat16 [512, 384], P('data', 'model')
- self_o: bfloat16 [384, 512], P('model', 'data')
- cross_q: bfloat16 [512, 384], P('data', 'model')
- cross_k: bfloat16 [512, 384], P('data', 'model')
- cross_v: bfloat16 [512, 384], P('data', 'model')
- cross_o: bfloat16 [384, 512], P('model', 'data')
- mlp_wi_0: bfloat16 [512, 1024], P('data', 'model')
- mlp_wi_1: bfloat16 [512, 1024], P('data', 'model')
- mlp_wo: bfloat16 [1024, 512], P('model', 'data')
- norm_self: bfloat16 [512], P('data')
- norm_cross: bfloat16 [512], P('data')
- norm_mlp: bfloat16 [512], P('data')
Outputs:
- output 1: bfloat16 [128, 384, 512], P('data')
- output 2: bfloat16 [128, 384, 512], P('data')
- output 3: bfloat16 [128, 192, 512], P('data')
- output 4: float32 [32, 6], P(None, 'model')
- output 5: float32 [512, 384], P('data', 'model')
- output 6: float32 [512, 384], P('data', 'model')
- output 7: float32 [512, 384], P('data', 'model')
- output 8: float32 [384, 512], P('model', 'data')
- output 9: float32 [512, 384], P('data', 'model')
- output 10: float32 [512, 384], P('data', 'model')
- output 11: float32 [512, 384], P('data', 'model')
- output 12: float32 [384, 512], P('model', 'data')
- output 13: float32 [512, 1024], P('data', 'model')
- output 14: float32 [512, 1024], P('data', 'model')
- output 15: float32 [1024, 512], P('model', 'data')
- output 16: float32 [512], P('data')
- output 17: float32 [512], P('data')
- output 18: float32 [512], P('data')
All inputs are finite; a program needn't handle non-finite values.
Results may differ from the reference program's by a relative error of at most 0.02.
Values are sent between devices in bfloat16 or wider.
A program may use at most 1 GiB of HBM per device.

```python
import math
import jax
import jax.numpy as jnp
from jax import lax

D = 512
HEADS = 6
HEAD = 64
FF = 1024
BATCH = 128
DEC_LEN = 384
ENC_LEN = 192
NUM_BUCKETS = 32
INNER = HEADS * HEAD
EPS = 1e-6
MASK_VALUE = -1e9
BUCKET_EDGES = tuple(math.ceil(16 * 8.0 ** (bucket_no / 16.0)) for bucket_no in range(1, 16))


def setup_inputs(seed: int = 0) -> dict:
    key_list = jax.random.split(jax.random.key(seed), 18)

    def normal(slot, arr_shape, factor):
        return (jax.random.normal(key_list[slot], arr_shape, jnp.float32) * factor).astype(jnp.bfloat16)

    def gain_draw(slot):
        return (1.0 + 0.3 * jax.random.normal(key_list[slot], (D,), jnp.float32)).astype(jnp.bfloat16)

    in_scale = D ** -0.5
    q_scale = (D * HEAD) ** -0.5
    out_scale = INNER ** -0.5
    return {
        "dec_in": normal(0, (BATCH, DEC_LEN, D), 1.0),
        "enc_out": normal(1, (BATCH, ENC_LEN, D), 1.0),
        "grad_out": normal(2, (BATCH, DEC_LEN, D), 1.0),
        "rel_bias": normal(3, (NUM_BUCKETS, HEADS), 1.5),
        "self_q": normal(4, (D, INNER), q_scale),
        "self_k": normal(5, (D, INNER), in_scale),
        "self_v": normal(6, (D, INNER), in_scale),
        "self_o": normal(7, (INNER, D), out_scale),
        "cross_q": normal(8, (D, INNER), q_scale),
        "cross_k": normal(9, (D, INNER), in_scale),
        "cross_v": normal(10, (D, INNER), in_scale),
        "cross_o": normal(11, (INNER, D), out_scale),
        "mlp_wi_0": normal(12, (D, FF), in_scale),
        "mlp_wi_1": normal(13, (D, FF), in_scale),
        "mlp_wo": normal(14, (FF, D), FF ** -0.5),
        "norm_self": gain_draw(15),
        "norm_cross": gain_draw(16),
        "norm_mlp": gain_draw(17),
    }


def to_bf(value_in):
    return value_in.astype(jnp.bfloat16).astype(jnp.float32)


def rms_norm(act_in, gain_vec):
    inv_rms = lax.rsqrt(jnp.mean(act_in * act_in, axis=-1, keepdims=True) + EPS)
    return to_bf(act_in * inv_rms * gain_vec)


def bucket_ids(seq_len):
    positions = jnp.arange(seq_len)
    rel_dist = jnp.maximum(positions[:, None] - positions[None, :], 0)
    bucket_edges = jnp.array(BUCKET_EDGES, dtype=jnp.int32)
    return jnp.minimum(rel_dist, 16) + jnp.sum((rel_dist[:, :, None] >= bucket_edges).astype(jnp.int32), axis=-1)


def project(act_in, weight):
    return to_bf(jnp.dot(act_in, weight, preferred_element_type=jnp.float32)).reshape(act_in.shape[0], HEADS, HEAD)


def attention(q_heads, k_heads, v_heads, pos_bias, key_mask):
    logits = to_bf(jnp.einsum("qhe,khe->hqk", q_heads, k_heads)) + pos_bias
    logits = jnp.where(key_mask, logits, MASK_VALUE)
    attn_probs = to_bf(jax.nn.softmax(logits, axis=-1))
    context = to_bf(jnp.einsum("hqk,khe->qhe", attn_probs, v_heads))
    return context.reshape(q_heads.shape[0], INNER)


def layer_seq(dec_seq, enc_seq, params):
    (rel_bias, self_q, self_k, self_v, self_o, cross_q, cross_k, cross_v, cross_o,
     mlp_wi_0, mlp_wi_1, mlp_wo, norm_self, norm_cross, norm_mlp) = params
    positions = jnp.arange(DEC_LEN)
    causal = positions[:, None] >= positions[None, :]
    pos_bias = jnp.transpose(rel_bias[bucket_ids(DEC_LEN)], (2, 0, 1))
    normed_1 = rms_norm(dec_seq, norm_self)
    ctx_self = attention(project(normed_1, self_q), project(normed_1, self_k), project(normed_1, self_v), pos_bias, causal)
    mid_1 = to_bf(dec_seq + jnp.dot(ctx_self, self_o, preferred_element_type=jnp.float32))
    normed_2 = rms_norm(mid_1, norm_cross)
    ctx_cross = attention(project(normed_2, cross_q), project(enc_seq, cross_k), project(enc_seq, cross_v), 0.0, True)
    mid_2 = to_bf(mid_1 + jnp.dot(ctx_cross, cross_o, preferred_element_type=jnp.float32))
    normed_3 = rms_norm(mid_2, norm_mlp)
    pre_0 = to_bf(jnp.dot(normed_3, mlp_wi_0, preferred_element_type=jnp.float32))
    pre_1 = to_bf(jnp.dot(normed_3, mlp_wi_1, preferred_element_type=jnp.float32))
    hidden = to_bf(jax.nn.gelu(pre_0, approximate=True) * pre_1)
    return to_bf(mid_2 + jnp.dot(hidden, mlp_wo, preferred_element_type=jnp.float32))


def reference(dec_in, enc_out, grad_out, rel_bias, self_q, self_k, self_v, self_o, cross_q, cross_k, cross_v, cross_o, mlp_wi_0, mlp_wi_1, mlp_wo, norm_self, norm_cross, norm_mlp):
    params = tuple(param_arr.astype(jnp.float32) for param_arr in (rel_bias, self_q, self_k, self_v, self_o, cross_q, cross_k, cross_v, cross_o, mlp_wi_0, mlp_wi_1, mlp_wo, norm_self, norm_cross, norm_mlp))

    def batch_step(grad_acc, seq_item):
        dec_seq, enc_seq, dy_seq = seq_item
        out_seq, pull_back = jax.vjp(layer_seq, dec_seq.astype(jnp.float32), enc_seq.astype(jnp.float32), params)
        d_dec, d_enc, d_params = pull_back(dy_seq.astype(jnp.float32))
        grad_acc = jax.tree.map(jnp.add, grad_acc, d_params)
        return grad_acc, (out_seq.astype(jnp.bfloat16), d_dec.astype(jnp.bfloat16), d_enc.astype(jnp.bfloat16))

    grad_zero = jax.tree.map(jnp.zeros_like, params)
    grad_sums, (dec_out, grad_dec, grad_enc) = lax.scan(batch_step, grad_zero, (dec_in, enc_out, grad_out))
    (g_bias, g_self_q, g_self_k, g_self_v, g_self_o, g_cross_q, g_cross_k, g_cross_v, g_cross_o,
     g_wi_0, g_wi_1, g_mlp_wo, g_norm_self, g_norm_cross, g_norm_mlp) = grad_sums
    return (dec_out, grad_dec, grad_enc, g_bias, g_self_q, g_self_k, g_self_v, g_self_o, g_cross_q, g_cross_k, g_cross_v, g_cross_o, g_wi_0, g_wi_1, g_mlp_wo, g_norm_self, g_norm_cross, g_norm_mlp)
```

```python
import math
import jax
import jax.numpy as jnp
from jax import lax
from jax.sharding import PartitionSpec as P

EPS = 1e-6
NUM_BUCKETS = 32
MASK_VALUE = -1e9
BUCKET_EDGES = tuple(math.ceil(16 * 8.0 ** (bucket_no / 16.0)) for bucket_no in range(1, 16))


def bucket_table(seq_len):
    positions = jnp.arange(seq_len)
    rel_dist = jnp.maximum(positions[:, None] - positions[None, :], 0)
    bucket_edges = jnp.array(BUCKET_EDGES, dtype=jnp.int32)
    bucket_ids = jnp.minimum(rel_dist, 16) + jnp.sum((rel_dist[:, :, None] >= bucket_edges).astype(jnp.int32), axis=-1)
    one_hot = (bucket_ids[:, :, None] == jnp.arange(NUM_BUCKETS)).astype(jnp.bfloat16)
    return one_hot, positions[:, None] >= positions[None, :]


def gelu_tanh(pre_act):
    return jax.nn.gelu(pre_act, approximate=True)


def norm_fwd(act_in, gain_vec):
    act_f = act_in.astype(jnp.float32)
    inv_rms = lax.rsqrt(jnp.mean(act_f * act_f, axis=-1, keepdims=True) + EPS)
    unit_act = act_f * inv_rms
    return (unit_act * gain_vec.astype(jnp.float32)).astype(jnp.bfloat16), unit_act, inv_rms


def norm_bwd(d_norm, unit_act, inv_rms, gain_vec):
    d_norm_f = d_norm.astype(jnp.float32)
    d_unit = d_norm_f * gain_vec.astype(jnp.float32)
    d_act = inv_rms * (d_unit - unit_act * jnp.mean(d_unit * unit_act, axis=-1, keepdims=True))
    return d_act, jnp.sum(d_norm_f * unit_act, axis=(0, 1))


def project(act_in, weight):
    return jnp.einsum("bsd,dhe->bshe", act_in, weight, preferred_element_type=jnp.float32).astype(jnp.bfloat16)


def back_in(d_heads, weight):
    return jnp.einsum("bshe,dhe->bsd", d_heads, weight, preferred_element_type=jnp.float32)


def in_grad(act_in, d_heads):
    grad_w = jnp.einsum("bsd,bshe->dhe", act_in, d_heads, preferred_element_type=jnp.float32)
    return grad_w.reshape(grad_w.shape[0], -1)


def out_proj(context, weight):
    return jnp.einsum("crif,ife->cre", context, weight, preferred_element_type=jnp.float32)


def out_grad(context, d_res):
    grad_w = jnp.einsum("crif,cre->ife", context, d_res, preferred_element_type=jnp.float32)
    return grad_w.reshape(-1, grad_w.shape[2])


def ctx_grad(d_res, weight):
    return jnp.einsum("cre,ife->crif", d_res, weight, preferred_element_type=jnp.float32).astype(jnp.bfloat16)


def attn_fwd(q_heads, k_heads, v_heads, pos_bias, key_mask):
    logits = jnp.einsum("bqhe,bkhe->bhqk", q_heads, k_heads, preferred_element_type=jnp.float32)
    logits = jnp.where(key_mask, logits.astype(jnp.bfloat16).astype(jnp.float32) + pos_bias, MASK_VALUE)
    attn_probs = jax.nn.softmax(logits, axis=-1)
    context = jnp.einsum("bhqk,bkhe->bqhe", attn_probs.astype(jnp.bfloat16), v_heads, preferred_element_type=jnp.float32)
    return attn_probs, context.astype(jnp.bfloat16)


def attn_bwd(d_context, attn_probs, q_heads, k_heads, v_heads):
    d_probs = jnp.einsum("bqhe,bkhe->bhqk", d_context, v_heads, preferred_element_type=jnp.float32)
    d_probs = d_probs.astype(jnp.bfloat16).astype(jnp.float32)
    d_logits = attn_probs * (d_probs - jnp.sum(attn_probs * d_probs, axis=-1, keepdims=True))
    d_logits_b = d_logits.astype(jnp.bfloat16)
    d_query = jnp.einsum("bhqk,bkhe->bqhe", d_logits_b, k_heads, preferred_element_type=jnp.float32)
    d_key = jnp.einsum("bhqk,bqhe->bkhe", d_logits_b, q_heads, preferred_element_type=jnp.float32)
    d_value = jnp.einsum("bhqk,bqhe->bkhe", attn_probs.astype(jnp.bfloat16), d_context, preferred_element_type=jnp.float32)
    return d_logits, d_query.astype(jnp.bfloat16), d_key.astype(jnp.bfloat16), d_value.astype(jnp.bfloat16)


def residual(base_val, delta_val):
    return (base_val.astype(jnp.float32) + delta_val.astype(jnp.float32)).astype(jnp.bfloat16)


IN_HALF = 192
FF_HALF = 512


def pack_local(sq, sk, sv, so, cq, ck, cv, co, wi0, wi1, wo):
    return [sq, sk, sv, so.T, cq, ck, cv, co.T, wi0, wi1, wo.T]


def gather_weights(blocks):
    local = jnp.concatenate(blocks, axis=1)
    pair = lax.all_gather(local, "model", axis=0)
    cols = []
    off = 0
    for blk in blocks:
        width = blk.shape[1]
        cols.append(pair[0, :, off:off + width])
        cols.append(pair[1, :, off:off + width])
        off += width
    both = jnp.concatenate(cols, axis=1)
    return lax.all_gather(both, "data", axis=0, tiled=True)


def scatter_grads(grad_all, widths):
    rows = lax.psum_scatter(grad_all, "data", scatter_dimension=0, tiled=True)
    lo, hi = [], []
    off = 0
    for width in widths:
        lo.append(rows[:, off:off + width])
        hi.append(rows[:, off + width:off + 2 * width])
        off += 2 * width
    pair = jnp.stack([jnp.concatenate(lo, axis=1), jnp.concatenate(hi, axis=1)])
    mine = lax.psum_scatter(pair, "model", scatter_dimension=0)
    outs = []
    off = 0
    for width in widths:
        outs.append(mine[:, off:off + width])
        off += width
    return outs


def layer_shard(dec_in, enc_out, grad_out, rel_bias, self_q, self_k, self_v, self_o, cross_q, cross_k, cross_v, cross_o, mlp_wi_0, mlp_wi_1, mlp_wo, norm_self, norm_cross, norm_mlp):
    model_idx = lax.axis_index("model")
    data_idx = lax.axis_index("data")
    half = dec_in.shape[0] // 2
    dec_in = lax.dynamic_slice_in_dim(dec_in, model_idx * half, half, 0)
    enc_out = lax.dynamic_slice_in_dim(enc_out, model_idx * half, half, 0)
    grad_out = lax.dynamic_slice_in_dim(grad_out, model_idx * half, half, 0)
    blocks = pack_local(self_q, self_k, self_v, self_o, cross_q, cross_k, cross_v, cross_o, mlp_wi_0, mlp_wi_1, mlp_wo)
    widths = [blk.shape[1] for blk in blocks]
    weights = gather_weights(blocks)
    full = []
    off = 0
    for width in widths:
        full.append(weights[:, off:off + 2 * width])
        off += 2 * width
    w_sq, w_sk, w_sv, w_so, w_cq, w_ck, w_cv, w_co, w_i0, w_i1, w_o = full
    gains = lax.all_gather(jnp.stack([norm_self, norm_cross, norm_mlp]), "data", axis=1, tiled=True)
    gain_1, gain_2, gain_3 = gains[0], gains[1], gains[2]
    bias_pair = lax.all_gather(rel_bias, "model", axis=1, tiled=True)

    heads = bias_pair.shape[1]
    one_hot, causal = bucket_table(dec_in.shape[1])
    pos_bias = jnp.einsum("qkr,rh->hqk", one_hot, bias_pair, preferred_element_type=jnp.float32)

    def heads_in(w):
        return w.reshape(w.shape[0], heads, -1)

    normed_1, unit_1, inv_1 = norm_fwd(dec_in, gain_1)
    q_self = project(normed_1, heads_in(w_sq))
    k_self = project(normed_1, heads_in(w_sk))
    v_self = project(normed_1, heads_in(w_sv))
    probs_self, ctx_self = attn_fwd(q_self, k_self, v_self, pos_bias, causal)
    mid_1 = residual(dec_in, back_in(ctx_self, heads_in(w_so)))

    normed_2, unit_2, inv_2 = norm_fwd(mid_1, gain_2)
    q_cross = project(normed_2, heads_in(w_cq))
    k_cross = project(enc_out, heads_in(w_ck))
    v_cross = project(enc_out, heads_in(w_cv))
    probs_cross, ctx_cross = attn_fwd(q_cross, k_cross, v_cross, 0.0, True)
    mid_2 = residual(mid_1, back_in(ctx_cross, heads_in(w_co)))

    normed_3, unit_3, inv_3 = norm_fwd(mid_2, gain_3)
    pre_0 = jnp.einsum("bsd,df->bsf", normed_3, w_i0, preferred_element_type=jnp.float32).astype(jnp.bfloat16)
    pre_1 = jnp.einsum("bsd,df->bsf", normed_3, w_i1, preferred_element_type=jnp.float32).astype(jnp.bfloat16)
    gelu_0, gelu_pull = jax.vjp(gelu_tanh, pre_0.astype(jnp.float32))
    hidden = (gelu_0 * pre_1.astype(jnp.float32)).astype(jnp.bfloat16)
    dec_out = residual(mid_2, jnp.einsum("bsf,df->bsd", hidden, w_o, preferred_element_type=jnp.float32))

    d_hidden = jnp.einsum("bsd,df->bsf", grad_out, w_o, preferred_element_type=jnp.float32)
    d_hidden = d_hidden.astype(jnp.bfloat16).astype(jnp.float32)
    d_pre_0 = gelu_pull(d_hidden * pre_1.astype(jnp.float32))[0].astype(jnp.bfloat16)
    d_pre_1 = (d_hidden * gelu_0).astype(jnp.bfloat16)
    d_norm_3 = (jnp.einsum("bsf,df->bsd", d_pre_0, w_i0, preferred_element_type=jnp.float32) + jnp.einsum("bsf,df->bsd", d_pre_1, w_i1, preferred_element_type=jnp.float32)).astype(jnp.bfloat16)

    def wgrad(act, d_out):
        return jnp.einsum("bsd,bsf->df", act, d_out, preferred_element_type=jnp.float32)

    g_wo = wgrad(grad_out, hidden)
    g_i0 = wgrad(normed_3, d_pre_0)
    g_i1 = wgrad(normed_3, d_pre_1)
    d_act_3, d_gain_3 = norm_bwd(d_norm_3, unit_3, inv_3, gain_3)
    d_mid_2 = residual(grad_out, d_act_3)

    g_co = in_grad(d_mid_2, ctx_cross)
    d_ctx_cross = project(d_mid_2, heads_in(w_co))
    _, dq_cross, dk_cross, dv_cross = attn_bwd(d_ctx_cross, probs_cross, q_cross, k_cross, v_cross)
    d_norm_2 = back_in(dq_cross, heads_in(w_cq)).astype(jnp.bfloat16)
    grad_enc = (back_in(dk_cross, heads_in(w_ck)) + back_in(dv_cross, heads_in(w_cv))).astype(jnp.bfloat16)
    g_cq = in_grad(normed_2, dq_cross)
    g_ck = in_grad(enc_out, dk_cross)
    g_cv = in_grad(enc_out, dv_cross)
    d_act_2, d_gain_2 = norm_bwd(d_norm_2, unit_2, inv_2, gain_2)
    d_mid_1 = residual(d_mid_2, d_act_2)

    g_so = in_grad(d_mid_1, ctx_self)
    d_ctx_self = project(d_mid_1, heads_in(w_so))
    d_logit_self, dq_self, dk_self, dv_self = attn_bwd(d_ctx_self, probs_self, q_self, k_self, v_self)
    bias_part = jnp.einsum("qkr,hqk->rh", one_hot.astype(jnp.float32), jnp.sum(d_logit_self, axis=0))
    d_norm_1 = (back_in(dq_self, heads_in(w_sq)) + back_in(dk_self, heads_in(w_sk)) + back_in(dv_self, heads_in(w_sv))).astype(jnp.bfloat16)
    g_sq = in_grad(normed_1, dq_self)
    g_sk = in_grad(normed_1, dk_self)
    g_sv = in_grad(normed_1, dv_self)
    d_act_1, d_gain_1 = norm_bwd(d_norm_1, unit_1, inv_1, gain_1)
    grad_dec = residual(d_mid_1, d_act_1)

    small = jnp.concatenate([d_gain_1, d_gain_2, d_gain_3, bias_part.reshape(-1)])
    small = lax.psum(small, ("model", "data"))
    gain_sums = small[:3 * gain_1.shape[0]].reshape(3, -1)
    gain_len = norm_self.shape[0]
    gain_mine = lax.dynamic_slice_in_dim(gain_sums, data_idx * gain_len, gain_len, 1)
    bias_sum = small[3 * gain_1.shape[0]:].reshape(bias_part.shape)
    grad_bias = lax.dynamic_slice_in_dim(bias_sum, model_idx * rel_bias.shape[1], rel_bias.shape[1], 1)

    grads = scatter_grads(jnp.concatenate([g_sq, g_sk, g_sv, g_so, g_cq, g_ck, g_cv, g_co, g_i0, g_i1, g_wo], axis=1), widths)
    o_sq, o_sk, o_sv, o_so, o_cq, o_ck, o_cv, o_co, o_i0, o_i1, o_wo = grads

    def both(arr):
        return lax.all_gather(arr, "model", axis=0, tiled=True)

    return (both(dec_out), both(grad_dec), both(grad_enc), grad_bias, o_sq, o_sk, o_sv, o_so.T, o_cq, o_ck, o_cv, o_co.T, o_i0, o_i1, o_wo.T, gain_mine[0], gain_mine[1], gain_mine[2])


def solution(mesh):
    row_spec = P("data", None, None)
    col_in = P("data", "model")
    col_out = P("model", "data")
    gain_spec = P("data")
    bias_spec = P(None, "model")
    arg_specs = (row_spec, row_spec, row_spec, bias_spec, col_in, col_in, col_in, col_out, col_in, col_in, col_in, col_out, col_in, col_in, col_out, gain_spec, gain_spec, gain_spec)
    out_specs = (row_spec, row_spec, row_spec) + arg_specs[3:]
    return jax.shard_map(layer_shard, mesh=mesh, in_specs=arg_specs, out_specs=out_specs, check_vma=False)
```

```python
import math
import jax
import jax.numpy as jnp
from jax import lax
from jax.experimental import pallas as pl
from jax.experimental.pallas import tpu as pltpu
from jax.sharding import PartitionSpec as P

EPS = 1e-6
NUM_BUCKETS = 32
MASK_VALUE = -1e9
BUCKET_EDGES = tuple(math.ceil(16 * 8.0 ** (bucket_no / 16.0)) for bucket_no in range(1, 16))


SEQ = 384
ENC = 192
DIM = 512
INNER = 384
FF = 1024
HEADS = 6
PAIRS = 3
QB = 128
CHUNK = 64
SEQS_STEP = 2
C_SQ, C_SO, C_CQ, C_CK, C_CO, C_I0, C_I1, C_WO, C_END = 0, 1152, 1536, 1920, 2688, 3072, 4096, 5120, 6144
BF = jnp.bfloat16
F32 = jnp.float32
GELU_C = math.sqrt(2.0 / math.pi)
GELU_K = 0.044715


def nn(a, b):
    return lax.dot_general(a, b, (((1,), (0,)), ((), ())), preferred_element_type=F32)


def nt(a, b):
    return lax.dot_general(a, b, (((1,), (1,)), ((), ())), preferred_element_type=F32)


def tn(a, b):
    return lax.dot_general(a, b, (((0,), (0,)), ((), ())), preferred_element_type=F32)


def unit_of(act_f):
    inv = lax.rsqrt(jnp.mean(act_f * act_f, axis=-1, keepdims=True) + EPS)
    return act_f * inv, inv


def head_mask(value, head, lane_idx):
    keep = (lane_idx < 64) if head == 0 else (lane_idx >= 64)
    return jnp.where(keep, value.astype(F32), 0.0).astype(BF)


def softmax_t(logits):
    top = jnp.max(logits, axis=0, keepdims=True)
    expd = jnp.exp(logits - top)
    return expd * (1.0 / jnp.sum(expd, axis=0, keepdims=True))


def seq_body(s, x_ref, e_ref, dy_ref, w_ref, gain_ref, bias_ref, y_ref, dx_ref, de_ref, dg_ref, db_ref,
             n1_s, n2_s, n3_s, dm1_s, dm2_s, qkv_s, dqkv_s, ctx_s, cq_s, ckv_s, dcq_s, dckv_s, cctx_s,
             hid_s, d01_s, x1_s, x2_s, dctx_s, pf_s, pt_s, cpf_s, cpt_s, ds_s, cds_s, km_s, vm_s):
    r0 = pl.multiple_of(s * SEQ, SEQ)
    e0 = pl.multiple_of(s * ENC, ENC)
    rows = pl.ds(r0, SEQ)
    erows = pl.ds(e0, ENC)

    def chunk_rows(off):
        return pl.ds(pl.multiple_of(r0 + off, CHUNK), CHUNK)

    chunks = range(0, SEQ, CHUNK)
    lane_idx = lax.broadcasted_iota(jnp.int32, (SEQ, QB), 1)
    tri = lax.broadcasted_iota(jnp.int32, (QB, QB), 0) <= lax.broadcasted_iota(jnp.int32, (QB, QB), 1)

    for off in chunks:
        unit, _ = unit_of(x_ref[chunk_rows(off), :].astype(F32))
        n1_s[chunk_rows(off), :] = (unit * gain_ref[0:1, :]).astype(BF)
    for col in range(0, 3 * INNER, INNER):
        qkv_s[:, col:col + INNER] = nn(n1_s[rows, :], w_ref[:, C_SQ + col:C_SQ + col + INNER]).astype(BF)

    def self_pair(hp, carry):
        o = pl.multiple_of(hp * QB, QB)
        k_pair = qkv_s[:, pl.ds(pl.multiple_of(INNER + o, QB), QB)]
        v_pair = qkv_s[:, pl.ds(pl.multiple_of(2 * INNER + o, QB), QB)]
        for head in range(2):
            km_s[head * SEQ:(head + 1) * SEQ, :] = head_mask(k_pair, head, lane_idx)
            vm_s[head * SEQ:(head + 1) * SEQ, :] = head_mask(v_pair, head, lane_idx)
        for head in range(2):
            for qb in range(3):
                n = QB * (qb + 1)
                logits = nt(km_s[head * SEQ:head * SEQ + n, :], qkv_s[qb * QB:(qb + 1) * QB, pl.ds(o, QB)])
                logits = logits.astype(BF).astype(F32) + bias_ref[2 * hp + head, SEQ - n:SEQ, :]
                diag = jnp.where(tri, logits[n - QB:n], MASK_VALUE)
                logits = diag if qb == 0 else jnp.concatenate([logits[:n - QB], diag], axis=0)
                probs = softmax_t(logits)
                pf_s[2 * hp + head, 0:n, qb * QB:(qb + 1) * QB] = probs
                pt_s[hp, head * SEQ:head * SEQ + n, qb * QB:(qb + 1) * QB] = probs.astype(BF)
        ctx_s[rows, pl.ds(o, QB)] = tn(pt_s[hp], vm_s[...]).astype(BF)
        return carry

    lax.fori_loop(0, PAIRS, self_pair, 0)

    delta = nt(ctx_s[rows, :], w_ref[:, C_SO:C_SO + INNER])
    for off in chunks:
        mid = (x_ref[chunk_rows(off), :].astype(F32) + delta[off:off + CHUNK]).astype(BF)
        x1_s[off:off + CHUNK, :] = mid
        unit, _ = unit_of(mid.astype(F32))
        n2_s[chunk_rows(off), :] = (unit * gain_ref[1:2, :]).astype(BF)
    cq_s[...] = nn(n2_s[rows, :], w_ref[:, C_CQ:C_CQ + INNER]).astype(BF)
    ckv_s[...] = nn(e_ref[erows, :], w_ref[:, C_CK:C_CK + 2 * INNER]).astype(BF)

    def cross_masks(o):
        k_pair = ckv_s[:, pl.ds(o, QB)]
        v_pair = ckv_s[:, pl.ds(pl.multiple_of(INNER + o, QB), QB)]
        for head in range(2):
            km_s[head * ENC:(head + 1) * ENC, :] = head_mask(k_pair, head, lane_idx[:ENC])
            vm_s[head * ENC:(head + 1) * ENC, :] = head_mask(v_pair, head, lane_idx[:ENC])

    def cross_pair(hp, carry):
        o = pl.multiple_of(hp * QB, QB)
        cross_masks(o)
        for head in range(2):
            for qb in range(3):
                cols = slice(qb * QB, (qb + 1) * QB)
                logits = nt(km_s[head * ENC:(head + 1) * ENC, :], cq_s[cols, pl.ds(o, QB)])
                probs = softmax_t(logits.astype(BF).astype(F32))
                cpf_s[2 * hp + head, :, cols] = probs
                cpt_s[hp, head * ENC:(head + 1) * ENC, cols] = probs.astype(BF)
        cctx_s[rows, pl.ds(o, QB)] = tn(cpt_s[hp], vm_s[0:2 * ENC, :]).astype(BF)
        return carry

    lax.fori_loop(0, PAIRS, cross_pair, 0)

    delta = nt(cctx_s[rows, :], w_ref[:, C_CO:C_CO + INNER])
    for off in chunks:
        mid = (x1_s[off:off + CHUNK, :].astype(F32) + delta[off:off + CHUNK]).astype(BF)
        x2_s[off:off + CHUNK, :] = mid
        unit, _ = unit_of(mid.astype(F32))
        n3_s[chunk_rows(off), :] = (unit * gain_ref[2:3, :]).astype(BF)
    step = 256
    for col in range(0, FF, step):
        pre_0 = nn(n3_s[rows, :], w_ref[:, C_I0 + col:C_I0 + col + step])
        pre_1 = nn(n3_s[rows, :], w_ref[:, C_I1 + col:C_I1 + col + step])
        d_hid = nn(dy_ref[rows, :], w_ref[:, C_WO + col:C_WO + col + step])
        for off in chunks:
            a0 = pre_0[off:off + CHUNK].astype(BF).astype(F32)
            a1 = pre_1[off:off + CHUNK].astype(BF).astype(F32)
            dh = d_hid[off:off + CHUNK].astype(BF).astype(F32)
            sq = a0 * a0
            half = 0.5 * jnp.tanh(a0 * (GELU_C + (GELU_C * GELU_K) * sq)) + 0.5
            gelu = a0 * half
            slope = half * (1.0 + (a0 - gelu) * (2.0 * GELU_C + (6.0 * GELU_C * GELU_K) * sq))
            hid_s[chunk_rows(off), col:col + step] = (gelu * a1).astype(BF)
            d01_s[chunk_rows(off), col:col + step] = (slope * (dh * a1)).astype(BF)
            d01_s[chunk_rows(off), FF + col:FF + col + step] = (dh * gelu).astype(BF)
    delta = nt(hid_s[rows, :], w_ref[:, C_WO:C_WO + FF])
    for off in chunks:
        y_ref[chunk_rows(off), :] = (x2_s[off:off + CHUNK, :].astype(F32) + delta[off:off + CHUNK]).astype(BF)

    def norm_back(d_norm, base, d_res, out, idx):
        total = dg_ref[8 * idx:8 * idx + 8, :]
        for off in chunks:
            d_n = d_norm[off:off + CHUNK].astype(BF).astype(F32)
            unit, inv = unit_of(base(off).astype(F32))
            total = total + jnp.sum((d_n * unit).reshape(CHUNK // 8, 8, DIM), axis=0)
            d_unit = d_n * gain_ref[idx:idx + 1, :]
            d_act = inv * (d_unit - unit * jnp.mean(d_unit * unit, axis=-1, keepdims=True))
            out[chunk_rows(off), :] = (d_res[chunk_rows(off), :].astype(F32) + d_act).astype(BF)
        dg_ref[8 * idx:8 * idx + 8, :] = total

    d_norm = nt(d01_s[rows, :], w_ref[:, C_I0:C_I0 + 2 * FF])
    norm_back(d_norm, lambda off: x2_s[off:off + CHUNK, :], dy_ref, dm2_s, 2)

    dctx_s[...] = nn(dm2_s[rows, :], w_ref[:, C_CO:C_CO + INNER]).astype(BF)

    def cross_pair_back(hp, carry):
        o = pl.multiple_of(hp * QB, QB)
        cross_masks(o)
        for head in range(2):
            for qb in range(3):
                cols = slice(qb * QB, (qb + 1) * QB)
                d_p = nt(vm_s[head * ENC:(head + 1) * ENC, :], dctx_s[cols, pl.ds(o, QB)]).astype(BF).astype(F32)
                probs = cpf_s[2 * hp + head, :, cols]
                d_l = probs * (d_p - jnp.sum(probs * d_p, axis=0, keepdims=True))
                cds_s[head * ENC:(head + 1) * ENC, cols] = d_l.astype(BF)
        dcq_s[rows, pl.ds(o, QB)] = tn(cds_s[...], km_s[0:2 * ENC, :]).astype(BF)
        d_k = nn(cds_s[...], cq_s[:, pl.ds(o, QB)])
        d_v = nn(cpt_s[hp], dctx_s[:, pl.ds(o, QB)])
        low = lane_idx[:ENC] < 64
        dckv_s[erows, pl.ds(o, QB)] = jnp.where(low, d_k[:ENC], d_k[ENC:]).astype(BF)
        dckv_s[erows, pl.ds(pl.multiple_of(INNER + o, QB), QB)] = jnp.where(low, d_v[:ENC], d_v[ENC:]).astype(BF)
        return carry

    lax.fori_loop(0, PAIRS, cross_pair_back, 0)
    d_norm = nt(dcq_s[rows, :], w_ref[:, C_CQ:C_CQ + INNER])
    de_ref[erows, :] = nt(dckv_s[erows, :], w_ref[:, C_CK:C_CK + 2 * INNER]).astype(BF)
    norm_back(d_norm, lambda off: x1_s[off:off + CHUNK, :], dm2_s, dm1_s, 1)

    dctx_s[...] = nn(dm1_s[rows, :], w_ref[:, C_SO:C_SO + INNER]).astype(BF)

    def self_pair_back(hp, carry):
        o = pl.multiple_of(hp * QB, QB)
        k_pair = qkv_s[:, pl.ds(pl.multiple_of(INNER + o, QB), QB)]
        v_pair = qkv_s[:, pl.ds(pl.multiple_of(2 * INNER + o, QB), QB)]
        for head in range(2):
            km_s[head * SEQ:(head + 1) * SEQ, :] = head_mask(k_pair, head, lane_idx)
            vm_s[head * SEQ:(head + 1) * SEQ, :] = head_mask(v_pair, head, lane_idx)
        for head in range(2):
            for qb in range(3):
                n = QB * (qb + 1)
                cols = slice(qb * QB, (qb + 1) * QB)
                d_p = nt(vm_s[head * SEQ:head * SEQ + n, :], dctx_s[cols, pl.ds(o, QB)]).astype(BF).astype(F32)
                probs = pf_s[2 * hp + head, 0:n, cols]
                d_l = probs * (d_p - jnp.sum(probs * d_p, axis=0, keepdims=True))
                db_ref[2 * hp + head, SEQ - n:SEQ, :] += d_l
                ds_s[head * SEQ:head * SEQ + n, cols] = d_l.astype(BF)
        dqkv_s[rows, pl.ds(o, QB)] = tn(ds_s[...], km_s[...]).astype(BF)
        d_k = nn(ds_s[...], qkv_s[:, pl.ds(o, QB)])
        d_v = nn(pt_s[hp], dctx_s[:, pl.ds(o, QB)])
        low = lane_idx < 64
        dqkv_s[rows, pl.ds(pl.multiple_of(INNER + o, QB), QB)] = jnp.where(low, d_k[:SEQ], d_k[SEQ:]).astype(BF)
        dqkv_s[rows, pl.ds(pl.multiple_of(2 * INNER + o, QB), QB)] = jnp.where(low, d_v[:SEQ], d_v[SEQ:]).astype(BF)
        return carry

    lax.fori_loop(0, PAIRS, self_pair_back, 0)
    d_norm = nt(dqkv_s[rows, :], w_ref[:, C_SQ:C_SQ + 3 * INNER])
    norm_back(d_norm, lambda off: x_ref[chunk_rows(off), :], dm1_s, dx_ref, 0)


SCRATCH = [
    ((2 * SEQ, DIM), BF),
    ((2 * SEQ, DIM), BF),
    ((2 * SEQ, DIM), BF),
    ((2 * SEQ, DIM), BF),
    ((2 * SEQ, DIM), BF),
    ((SEQ, 3 * INNER), BF),
    ((2 * SEQ, 3 * INNER), BF),
    ((2 * SEQ, INNER), BF),
    ((SEQ, INNER), BF),
    ((ENC, 2 * INNER), BF),
    ((2 * SEQ, INNER), BF),
    ((2 * ENC, 2 * INNER), BF),
    ((2 * SEQ, INNER), BF),
    ((2 * SEQ, FF), BF),
    ((2 * SEQ, 2 * FF), BF),
    ((SEQ, DIM), BF),
    ((SEQ, DIM), BF),
    ((SEQ, INNER), BF),
    ((HEADS, SEQ, SEQ), F32),
    ((PAIRS, 2 * SEQ, SEQ), BF),
    ((HEADS, ENC, SEQ), F32),
    ((PAIRS, 2 * ENC, SEQ), BF),
    ((2 * SEQ, SEQ), BF),
    ((2 * ENC, SEQ), BF),
    ((2 * SEQ, QB), BF),
    ((2 * SEQ, QB), BF),
]


def weight_grads(g_ref, e_ref, dy_ref, n1_s, n2_s, n3_s, dm1_s, dm2_s, dqkv_s, ctx_s, dcq_s, dckv_s, cctx_s, hid_s, d01_s):
    def add(act, d_out, col, width):
        for off in range(0, width, 384 if width % 384 == 0 else 512):
            size = 384 if width % 384 == 0 else 512
            g_ref[:, col + off:col + off + size] += tn(act[...], d_out[:, off:off + size])

    add(n3_s, d01_s, C_I0, 2 * FF)
    add(dy_ref, hid_s, C_WO, FF)
    add(dm2_s, cctx_s, C_CO, INNER)
    add(n2_s, dcq_s, C_CQ, INNER)
    add(e_ref, dckv_s, C_CK, 2 * INNER)
    add(dm1_s, ctx_s, C_SO, INNER)
    add(n1_s, dqkv_s, C_SQ, 3 * INNER)


def layer_kernel(x_ref, e_ref, dy_ref, w_ref, gain_ref, bias_ref, y_ref, dx_ref, de_ref, g_ref, dg_ref, db_ref, *scratch):
    (n1_s, n2_s, n3_s, dm1_s, dm2_s, qkv_s, dqkv_s, ctx_s, cq_s, ckv_s, dcq_s, dckv_s, cctx_s,
     hid_s, d01_s, x1_s, x2_s, dctx_s, pf_s, pt_s, cpf_s, cpt_s, ds_s, cds_s, km_s, vm_s) = scratch

    @pl.when(pl.program_id(0) == 0)
    def _():
        pt_s[...] = jnp.zeros_like(pt_s)
        ds_s[...] = jnp.zeros_like(ds_s)
        dg_ref[...] = jnp.zeros_like(dg_ref)
        db_ref[...] = jnp.zeros_like(db_ref)
        g_ref[...] = jnp.zeros_like(g_ref)

    def body(s, carry):
        seq_body(s, x_ref, e_ref, dy_ref, w_ref, gain_ref, bias_ref, y_ref, dx_ref, de_ref, dg_ref, db_ref, *scratch)
        return carry

    lax.fori_loop(0, SEQS_STEP, body, 0)
    weight_grads(g_ref, e_ref, dy_ref, n1_s, n2_s, n3_s, dm1_s, dm2_s, dqkv_s, ctx_s, dcq_s, dckv_s, cctx_s, hid_s, d01_s)


def pack_local(sq, sk, sv, so, cq, ck, cv, co, wi0, wi1, wo):
    return [sq, sk, sv, so.T, cq, ck, cv, co.T, wi0, wi1, wo.T]


def gather_weights(blocks):
    local = jnp.concatenate(blocks, axis=1)
    pair = lax.all_gather(local, "model", axis=0)
    cols = []
    off = 0
    for blk in blocks:
        width = blk.shape[1]
        cols.append(pair[0, :, off:off + width])
        cols.append(pair[1, :, off:off + width])
        off += width
    both = jnp.concatenate(cols, axis=1)
    return lax.all_gather(both, "data", axis=0, tiled=True)


def scatter_grads(grad_all, widths):
    rows = lax.psum_scatter(grad_all, "data", scatter_dimension=0, tiled=True)
    lo, hi = [], []
    off = 0
    for width in widths:
        lo.append(rows[:, off:off + width])
        hi.append(rows[:, off + width:off + 2 * width])
        off += 2 * width
    pair = jnp.stack([jnp.concatenate(lo, axis=1), jnp.concatenate(hi, axis=1)])
    mine = lax.psum_scatter(pair, "model", scatter_dimension=0)
    outs = []
    off = 0
    for width in widths:
        outs.append(mine[:, off:off + width])
        off += width
    return outs


def layer_call(x, e, dy, weights, gains, bias_t):
    steps = x.shape[0] // (SEQS_STEP * SEQ)
    blk = lambda rows: pl.BlockSpec((rows, DIM), lambda i: (i, 0))
    fixed = lambda arr_shape: pl.BlockSpec(arr_shape, lambda i: (0,) * len(arr_shape), pipeline_mode=pl.Buffered(1))
    rows, erows = SEQS_STEP * SEQ, SEQS_STEP * ENC
    outs = [jax.ShapeDtypeStruct(x.shape, BF), jax.ShapeDtypeStruct(x.shape, BF), jax.ShapeDtypeStruct(e.shape, BF),
            jax.ShapeDtypeStruct((DIM, C_END), F32), jax.ShapeDtypeStruct((24, DIM), F32), jax.ShapeDtypeStruct((HEADS, SEQ, QB), F32)]
    return pl.pallas_call(
        layer_kernel,
        out_shape=outs,
        grid=(steps,),
        in_specs=[blk(rows), blk(erows), blk(rows), fixed(weights.shape), fixed(gains.shape), fixed(bias_t.shape)],
        out_specs=[blk(rows), blk(rows), blk(erows), fixed((DIM, C_END)), fixed((24, DIM)), fixed((HEADS, SEQ, QB))],
        scratch_shapes=[pltpu.VMEM(*item) for item in SCRATCH],
        compiler_params=pltpu.CompilerParams(dimension_semantics=("arbitrary",), vmem_limit_bytes=67043328),
        name="layer",
    )(x, e, dy, weights, gains, bias_t)


def bias_table():
    dist = (SEQ - QB + jnp.arange(QB))[None, :] - jnp.arange(SEQ)[:, None]
    dist = jnp.maximum(dist, 0)
    edges = jnp.array(BUCKET_EDGES, dtype=jnp.int32)
    ids = jnp.minimum(dist, 16) + jnp.sum((dist[:, :, None] >= edges).astype(jnp.int32), axis=-1)
    return ids


def layer_shard(dec_in, enc_out, grad_out, rel_bias, self_q, self_k, self_v, self_o, cross_q, cross_k, cross_v, cross_o, mlp_wi_0, mlp_wi_1, mlp_wo, norm_self, norm_cross, norm_mlp):
    model_idx = lax.axis_index("model")
    data_idx = lax.axis_index("data")
    half = dec_in.shape[0] // 2

    def mine(arr):
        part = lax.dynamic_slice_in_dim(arr, model_idx * half, half, 0)
        return part.reshape(-1, arr.shape[2])

    blocks = pack_local(self_q, self_k, self_v, self_o, cross_q, cross_k, cross_v, cross_o, mlp_wi_0, mlp_wi_1, mlp_wo)
    widths = [blk.shape[1] for blk in blocks]
    weights = gather_weights(blocks)
    gains = lax.all_gather(jnp.stack([norm_self, norm_cross, norm_mlp]), "data", axis=1, tiled=True).astype(F32)
    bias_pair = lax.all_gather(rel_bias, "model", axis=1, tiled=True).astype(F32)
    ids = bias_table()
    hot = (ids[:, :, None] == jnp.arange(NUM_BUCKETS)).astype(F32)
    bias_t = jnp.einsum("car,rh->hca", hot, bias_pair, precision=lax.Precision.HIGHEST)
    dec_out, grad_dec, grad_enc, grad_all, gain_part, bias_rows = layer_call(mine(dec_in), mine(enc_out), mine(grad_out), weights, gains, bias_t)
    bias_part = jnp.einsum("car,hca->rh", hot, bias_rows, precision=lax.Precision.HIGHEST)
    gain_part = jnp.sum(gain_part.reshape(3, 8, DIM), axis=1)

    small = jnp.concatenate([gain_part.reshape(-1), bias_part.reshape(-1)])
    small = lax.psum(small, ("model", "data"))
    gain_sums = small[:3 * DIM].reshape(3, DIM)
    gain_len = norm_self.shape[0]
    gain_mine = lax.dynamic_slice_in_dim(gain_sums, data_idx * gain_len, gain_len, 1)
    bias_sum = small[3 * DIM:].reshape(bias_part.shape)
    grad_bias = lax.dynamic_slice_in_dim(bias_sum, model_idx * rel_bias.shape[1], rel_bias.shape[1], 1)

    o_sq, o_sk, o_sv, o_so, o_cq, o_ck, o_cv, o_co, o_i0, o_i1, o_wo = scatter_grads(grad_all, widths)

    def both(arr, length):
        return lax.all_gather(arr.reshape(half, length, DIM), "model", axis=0, tiled=True)

    return (both(dec_out, SEQ), both(grad_dec, SEQ), both(grad_enc, ENC), grad_bias, o_sq, o_sk, o_sv, o_so.T, o_cq, o_ck, o_cv, o_co.T, o_i0, o_i1, o_wo.T, gain_mine[0], gain_mine[1], gain_mine[2])


def solution(mesh):
    row_spec = P("data", None, None)
    col_in = P("data", "model")
    col_out = P("model", "data")
    gain_spec = P("data")
    bias_spec = P(None, "model")
    arg_specs = (row_spec, row_spec, row_spec, bias_spec, col_in, col_in, col_in, col_out, col_in, col_in, col_in, col_out, col_in, col_in, col_out, gain_spec, gain_spec, gain_spec)
    out_specs = (row_spec, row_spec, row_spec) + arg_specs[3:]
    return jax.shard_map(layer_shard, mesh=mesh, in_specs=arg_specs, out_specs=out_specs, check_vma=False)
```

```python
import math
import jax
import jax.numpy as jnp
from jax import lax
from jax.experimental import pallas as pl
from jax.experimental.pallas import tpu as pltpu
from jax.sharding import PartitionSpec as P

EPS = 1e-6
NUM_BUCKETS = 32
MASK_VALUE = -1e9
BUCKET_EDGES = tuple(math.ceil(16 * 8.0 ** (bucket_no / 16.0)) for bucket_no in range(1, 16))


SEQ = 384
ENC = 192
DIM = 512
INNER = 384
FF = 1024
HEADS = 6
PAIRS = 3
QB = 128
CHUNK = 64
SEQS_STEP = 2
C_SQ, C_SO, C_CQ, C_CK, C_CO, C_I0, C_I1, C_WO, C_END = 0, 1152, 1536, 1920, 2688, 3072, 4096, 5120, 6144
BF = jnp.bfloat16
F32 = jnp.float32
GELU_C = math.sqrt(2.0 / math.pi)
GELU_K = 0.044715
MESH = pl.DeviceIdType.MESH


def nn(a, b):
    return lax.dot_general(a, b, (((1,), (0,)), ((), ())), preferred_element_type=F32)


def nt(a, b):
    return lax.dot_general(a, b, (((1,), (1,)), ((), ())), preferred_element_type=F32)


def tn(a, b):
    return lax.dot_general(a, b, (((0,), (0,)), ((), ())), preferred_element_type=F32)


def unit_of(act_f):
    inv = lax.rsqrt(jnp.mean(act_f * act_f, axis=-1, keepdims=True) + EPS)
    return act_f * inv, inv


def head_mask(value, head, lane_idx):
    keep = (lane_idx < 64) if head == 0 else (lane_idx >= 64)
    return jnp.where(keep, value.astype(F32), 0.0).astype(BF)


def softmax_t(logits):
    top = jnp.max(logits, axis=0, keepdims=True)
    expd = jnp.exp(logits - top)
    return expd * (1.0 / jnp.sum(expd, axis=0, keepdims=True))


def seq_body(s, exchange, x_ref, e_ref, dy_ref, w_ref, gain_ref, bias_ref, y_buf, dx_buf, de_buf, dg_ref, db_ref,
             n1_s, n2_s, n3_s, dm1_s, dm2_s, qkv_s, dqkv_s, ctx_s, cq_s, ckv_s, dcq_s, dckv_s, cctx_s,
             hid_s, d01_s, x1_s, x2_s, dctx_s, pf_s, pt_s, cpf_s, cpt_s, ds_s, cds_s, km_s, vm_s):
    r0 = pl.multiple_of(s * SEQ, SEQ)
    e0 = pl.multiple_of(s * ENC, ENC)
    rows = pl.ds(r0, SEQ)
    erows = pl.ds(e0, ENC)

    def chunk_rows(off):
        return pl.ds(pl.multiple_of(r0 + off, CHUNK), CHUNK)

    chunks = range(0, SEQ, CHUNK)
    slot, wait_slot, send = exchange
    lane_idx = lax.broadcasted_iota(jnp.int32, (SEQ, QB), 1)
    tri = lax.broadcasted_iota(jnp.int32, (QB, QB), 0) <= lax.broadcasted_iota(jnp.int32, (QB, QB), 1)

    for off in chunks:
        unit, _ = unit_of(x_ref[chunk_rows(off), :].astype(F32))
        n1_s[chunk_rows(off), :] = (unit * gain_ref[0:1, :]).astype(BF)
    for col in range(0, 3 * INNER, INNER):
        qkv_s[:, col:col + INNER] = nn(n1_s[rows, :], w_ref[:, C_SQ + col:C_SQ + col + INNER]).astype(BF)

    def self_pair(hp, carry):
        o = pl.multiple_of(hp * QB, QB)
        k_pair = qkv_s[:, pl.ds(pl.multiple_of(INNER + o, QB), QB)]
        v_pair = qkv_s[:, pl.ds(pl.multiple_of(2 * INNER + o, QB), QB)]
        for head in range(2):
            km_s[head * SEQ:(head + 1) * SEQ, :] = head_mask(k_pair, head, lane_idx)
            vm_s[head * SEQ:(head + 1) * SEQ, :] = head_mask(v_pair, head, lane_idx)
        for head in range(2):
            for qb in range(3):
                n = QB * (qb + 1)
                logits = nt(km_s[head * SEQ:head * SEQ + n, :], qkv_s[qb * QB:(qb + 1) * QB, pl.ds(o, QB)])
                logits = logits.astype(BF).astype(F32) + bias_ref[2 * hp + head, SEQ - n:SEQ, :]
                diag = jnp.where(tri, logits[n - QB:n], MASK_VALUE)
                logits = diag if qb == 0 else jnp.concatenate([logits[:n - QB], diag], axis=0)
                probs = softmax_t(logits)
                pf_s[2 * hp + head, 0:n, qb * QB:(qb + 1) * QB] = probs
                pt_s[hp, head * SEQ:head * SEQ + n, qb * QB:(qb + 1) * QB] = probs.astype(BF)
        ctx_s[rows, pl.ds(o, QB)] = tn(pt_s[hp], vm_s[...]).astype(BF)
        return carry

    lax.fori_loop(0, PAIRS, self_pair, 0)

    delta = nt(ctx_s[rows, :], w_ref[:, C_SO:C_SO + INNER])
    for off in chunks:
        mid = (x_ref[chunk_rows(off), :].astype(F32) + delta[off:off + CHUNK]).astype(BF)
        x1_s[off:off + CHUNK, :] = mid
        unit, _ = unit_of(mid.astype(F32))
        n2_s[chunk_rows(off), :] = (unit * gain_ref[1:2, :]).astype(BF)
    cq_s[...] = nn(n2_s[rows, :], w_ref[:, C_CQ:C_CQ + INNER]).astype(BF)
    ckv_s[...] = nn(e_ref[erows, :], w_ref[:, C_CK:C_CK + 2 * INNER]).astype(BF)

    def cross_masks(o):
        k_pair = ckv_s[:, pl.ds(o, QB)]
        v_pair = ckv_s[:, pl.ds(pl.multiple_of(INNER + o, QB), QB)]
        for head in range(2):
            km_s[head * ENC:(head + 1) * ENC, :] = head_mask(k_pair, head, lane_idx[:ENC])
            vm_s[head * ENC:(head + 1) * ENC, :] = head_mask(v_pair, head, lane_idx[:ENC])

    def cross_pair(hp, carry):
        o = pl.multiple_of(hp * QB, QB)
        cross_masks(o)
        for head in range(2):
            for qb in range(3):
                cols = slice(qb * QB, (qb + 1) * QB)
                logits = nt(km_s[head * ENC:(head + 1) * ENC, :], cq_s[cols, pl.ds(o, QB)])
                probs = softmax_t(logits.astype(BF).astype(F32))
                cpf_s[2 * hp + head, :, cols] = probs
                cpt_s[hp, head * ENC:(head + 1) * ENC, cols] = probs.astype(BF)
        cctx_s[rows, pl.ds(o, QB)] = tn(cpt_s[hp], vm_s[0:2 * ENC, :]).astype(BF)
        return carry

    lax.fori_loop(0, PAIRS, cross_pair, 0)

    delta = nt(cctx_s[rows, :], w_ref[:, C_CO:C_CO + INNER])
    for off in chunks:
        mid = (x1_s[off:off + CHUNK, :].astype(F32) + delta[off:off + CHUNK]).astype(BF)
        x2_s[off:off + CHUNK, :] = mid
        unit, _ = unit_of(mid.astype(F32))
        n3_s[chunk_rows(off), :] = (unit * gain_ref[2:3, :]).astype(BF)
    step = 256
    for col in range(0, FF, step):
        pre_0 = nn(n3_s[rows, :], w_ref[:, C_I0 + col:C_I0 + col + step])
        pre_1 = nn(n3_s[rows, :], w_ref[:, C_I1 + col:C_I1 + col + step])
        d_hid = nn(dy_ref[rows, :], w_ref[:, C_WO + col:C_WO + col + step])
        for off in chunks:
            a0 = pre_0[off:off + CHUNK].astype(BF).astype(F32)
            a1 = pre_1[off:off + CHUNK].astype(BF).astype(F32)
            dh = d_hid[off:off + CHUNK].astype(BF).astype(F32)
            sq = a0 * a0
            half = 0.5 * jnp.tanh(a0 * (GELU_C + (GELU_C * GELU_K) * sq)) + 0.5
            gelu = a0 * half
            slope = half * (1.0 + (a0 - gelu) * (2.0 * GELU_C + (6.0 * GELU_C * GELU_K) * sq))
            hid_s[chunk_rows(off), col:col + step] = (gelu * a1).astype(BF)
            d01_s[chunk_rows(off), col:col + step] = (slope * (dh * a1)).astype(BF)
            d01_s[chunk_rows(off), FF + col:FF + col + step] = (dh * gelu).astype(BF)
    delta = nt(hid_s[rows, :], w_ref[:, C_WO:C_WO + FF])
    wait_slot(0)
    for off in chunks:
        y_buf[slot, off:off + CHUNK, :] = (x2_s[off:off + CHUNK, :].astype(F32) + delta[off:off + CHUNK]).astype(BF)
    send(0)

    def norm_back(d_norm, base, d_res, out, idx):
        total = dg_ref[8 * idx:8 * idx + 8, :]
        for off in chunks:
            d_n = d_norm[off:off + CHUNK].astype(BF).astype(F32)
            unit, inv = unit_of(base(off).astype(F32))
            total = total + jnp.sum((d_n * unit).reshape(CHUNK // 8, 8, DIM), axis=0)
            d_unit = d_n * gain_ref[idx:idx + 1, :]
            d_act = inv * (d_unit - unit * jnp.mean(d_unit * unit, axis=-1, keepdims=True))
            out(off)[...] = (d_res[chunk_rows(off), :].astype(F32) + d_act).astype(BF)
        dg_ref[8 * idx:8 * idx + 8, :] = total

    d_norm = nt(d01_s[rows, :], w_ref[:, C_I0:C_I0 + 2 * FF])
    norm_back(d_norm, lambda off: x2_s[off:off + CHUNK, :], dy_ref, lambda off: dm2_s.at[chunk_rows(off), :], 2)

    dctx_s[...] = nn(dm2_s[rows, :], w_ref[:, C_CO:C_CO + INNER]).astype(BF)

    def cross_pair_back(hp, carry):
        o = pl.multiple_of(hp * QB, QB)
        cross_masks(o)
        for head in range(2):
            for qb in range(3):
                cols = slice(qb * QB, (qb + 1) * QB)
                d_p = nt(vm_s[head * ENC:(head + 1) * ENC, :], dctx_s[cols, pl.ds(o, QB)]).astype(BF).astype(F32)
                probs = cpf_s[2 * hp + head, :, cols]
                d_l = probs * (d_p - jnp.sum(probs * d_p, axis=0, keepdims=True))
                cds_s[head * ENC:(head + 1) * ENC, cols] = d_l.astype(BF)
        dcq_s[rows, pl.ds(o, QB)] = tn(cds_s[...], km_s[0:2 * ENC, :]).astype(BF)
        d_k = nn(cds_s[...], cq_s[:, pl.ds(o, QB)])
        d_v = nn(cpt_s[hp], dctx_s[:, pl.ds(o, QB)])
        low = lane_idx[:ENC] < 64
        dckv_s[erows, pl.ds(o, QB)] = jnp.where(low, d_k[:ENC], d_k[ENC:]).astype(BF)
        dckv_s[erows, pl.ds(pl.multiple_of(INNER + o, QB), QB)] = jnp.where(low, d_v[:ENC], d_v[ENC:]).astype(BF)
        return carry

    lax.fori_loop(0, PAIRS, cross_pair_back, 0)
    d_norm = nt(dcq_s[rows, :], w_ref[:, C_CQ:C_CQ + INNER])
    wait_slot(2)
    de_buf[slot] = nt(dckv_s[erows, :], w_ref[:, C_CK:C_CK + 2 * INNER]).astype(BF)
    send(2)
    norm_back(d_norm, lambda off: x1_s[off:off + CHUNK, :], dm2_s, lambda off: dm1_s.at[chunk_rows(off), :], 1)

    dctx_s[...] = nn(dm1_s[rows, :], w_ref[:, C_SO:C_SO + INNER]).astype(BF)

    def self_pair_back(hp, carry):
        o = pl.multiple_of(hp * QB, QB)
        k_pair = qkv_s[:, pl.ds(pl.multiple_of(INNER + o, QB), QB)]
        v_pair = qkv_s[:, pl.ds(pl.multiple_of(2 * INNER + o, QB), QB)]
        for head in range(2):
            km_s[head * SEQ:(head + 1) * SEQ, :] = head_mask(k_pair, head, lane_idx)
            vm_s[head * SEQ:(head + 1) * SEQ, :] = head_mask(v_pair, head, lane_idx)
        for head in range(2):
            for qb in range(3):
                n = QB * (qb + 1)
                cols = slice(qb * QB, (qb + 1) * QB)
                d_p = nt(vm_s[head * SEQ:head * SEQ + n, :], dctx_s[cols, pl.ds(o, QB)]).astype(BF).astype(F32)
                probs = pf_s[2 * hp + head, 0:n, cols]
                d_l = probs * (d_p - jnp.sum(probs * d_p, axis=0, keepdims=True))
                db_ref[2 * hp + head, SEQ - n:SEQ, :] += d_l
                ds_s[head * SEQ:head * SEQ + n, cols] = d_l.astype(BF)
        dqkv_s[rows, pl.ds(o, QB)] = tn(ds_s[...], km_s[...]).astype(BF)
        d_k = nn(ds_s[...], qkv_s[:, pl.ds(o, QB)])
        d_v = nn(pt_s[hp], dctx_s[:, pl.ds(o, QB)])
        low = lane_idx < 64
        dqkv_s[rows, pl.ds(pl.multiple_of(INNER + o, QB), QB)] = jnp.where(low, d_k[:SEQ], d_k[SEQ:]).astype(BF)
        dqkv_s[rows, pl.ds(pl.multiple_of(2 * INNER + o, QB), QB)] = jnp.where(low, d_v[:SEQ], d_v[SEQ:]).astype(BF)
        return carry

    lax.fori_loop(0, PAIRS, self_pair_back, 0)
    d_norm = nt(dqkv_s[rows, :], w_ref[:, C_SQ:C_SQ + 3 * INNER])
    wait_slot(1)
    norm_back(d_norm, lambda off: x_ref[chunk_rows(off), :], dm1_s, lambda off: dx_buf.at[slot, off:off + CHUNK, :], 0)
    send(1)


SCRATCH = [
    ((2 * SEQ, DIM), BF),
    ((2 * SEQ, DIM), BF),
    ((2 * SEQ, DIM), BF),
    ((2 * SEQ, DIM), BF),
    ((2 * SEQ, DIM), BF),
    ((SEQ, 3 * INNER), BF),
    ((2 * SEQ, 3 * INNER), BF),
    ((2 * SEQ, INNER), BF),
    ((SEQ, INNER), BF),
    ((ENC, 2 * INNER), BF),
    ((2 * SEQ, INNER), BF),
    ((2 * ENC, 2 * INNER), BF),
    ((2 * SEQ, INNER), BF),
    ((2 * SEQ, FF), BF),
    ((2 * SEQ, 2 * FF), BF),
    ((SEQ, DIM), BF),
    ((SEQ, DIM), BF),
    ((SEQ, INNER), BF),
    ((HEADS, SEQ, SEQ), F32),
    ((PAIRS, 2 * SEQ, SEQ), BF),
    ((HEADS, ENC, SEQ), F32),
    ((PAIRS, 2 * ENC, SEQ), BF),
    ((2 * SEQ, SEQ), BF),
    ((2 * ENC, SEQ), BF),
    ((2 * SEQ, QB), BF),
    ((2 * SEQ, QB), BF),
]


def weight_grads(g_ref, e_ref, dy_ref, n1_s, n2_s, n3_s, dm1_s, dm2_s, dqkv_s, ctx_s, dcq_s, dckv_s, cctx_s, hid_s, d01_s):
    def add(act, d_out, col, width):
        for off in range(0, width, 384 if width % 384 == 0 else 512):
            size = 384 if width % 384 == 0 else 512
            g_ref[:, col + off:col + off + size] += tn(act[...], d_out[:, off:off + size])

    add(n3_s, d01_s, C_I0, 2 * FF)
    add(dy_ref, hid_s, C_WO, FF)
    add(dm2_s, cctx_s, C_CO, INNER)
    add(n2_s, dcq_s, C_CQ, INNER)
    add(e_ref, dckv_s, C_CK, 2 * INNER)
    add(dm1_s, ctx_s, C_SO, INNER)
    add(n1_s, dqkv_s, C_SQ, 3 * INNER)


def layer_kernel(x_ref, e_ref, dy_ref, w_ref, gain_ref, bias_ref, y_hbm, dx_hbm, de_hbm, g_ref, dg_ref, db_ref, *scratch):
    *scratch, y_buf, dx_buf, de_buf, local_sem, send_sem, recv_sem = scratch
    (n1_s, n2_s, n3_s, dm1_s, dm2_s, qkv_s, dqkv_s, ctx_s, cq_s, ckv_s, dcq_s, dckv_s, cctx_s,
     hid_s, d01_s, x1_s, x2_s, dctx_s, pf_s, pt_s, cpf_s, cpt_s, ds_s, cds_s, km_s, vm_s) = scratch
    me = lax.axis_index("model")
    other = 1 - me
    step = pl.program_id(0)
    seqs = SEQS_STEP * pl.num_programs(0)
    bufs = ((y_buf, y_hbm, SEQ), (dx_buf, dx_hbm, SEQ), (de_buf, de_hbm, ENC))

    @pl.when(step == 0)
    def _():
        barrier = pltpu.get_barrier_semaphore()
        pl.semaphore_signal(barrier, inc=1, device_id={"model": other}, device_id_type=MESH)
        pl.semaphore_wait(barrier, 1)
        pt_s[...] = jnp.zeros_like(pt_s)
        ds_s[...] = jnp.zeros_like(ds_s)
        dg_ref[...] = jnp.zeros_like(dg_ref)
        db_ref[...] = jnp.zeros_like(db_ref)
        g_ref[...] = jnp.zeros_like(g_ref)

    def copies(which, number):
        buf, hbm, length = bufs[which]
        slot = lax.rem(number, 2)
        rows = pl.ds(pl.multiple_of((me * seqs + number) * length, length), length)
        local = pltpu.make_async_copy(buf.at[slot], hbm.at[rows, :], local_sem.at[which, slot])
        remote = pltpu.make_async_remote_copy(
            src_ref=buf.at[slot], dst_ref=hbm.at[rows, :], send_sem=send_sem.at[which, slot],
            recv_sem=recv_sem.at[which, number], device_id={"model": other}, device_id_type=MESH)
        return local, remote

    def body(s, carry):
        number = step * SEQS_STEP + s

        def wait_slot(which):
            @pl.when(number >= 2)
            def _():
                local, remote = copies(which, number - 2)
                local.wait()
                remote.wait_send()

        def send(which):
            local, remote = copies(which, number)
            remote.start()
            local.start()

        seq_body(s, (lax.rem(number, 2), wait_slot, send), x_ref, e_ref, dy_ref, w_ref, gain_ref, bias_ref, y_buf, dx_buf, de_buf, dg_ref, db_ref, *scratch)
        return carry

    lax.fori_loop(0, SEQS_STEP, body, 0)
    weight_grads(g_ref, e_ref, dy_ref, n1_s, n2_s, n3_s, dm1_s, dm2_s, dqkv_s, ctx_s, dcq_s, dckv_s, cctx_s, hid_s, d01_s)

    @pl.when(step == pl.num_programs(0) - 1)
    def _():
        for which in range(3):
            for back in (2, 1):
                local, remote = copies(which, seqs - back)
                local.wait()
                remote.wait_send()

            def arrived(number, carry):
                copies(which, number)[1].wait_recv()
                return carry

            lax.fori_loop(0, seqs, arrived, 0)


def pack_local(sq, sk, sv, so, cq, ck, cv, co, wi0, wi1, wo):
    return [sq, sk, sv, so.T, cq, ck, cv, co.T, wi0, wi1, wo.T]


def gather_weights(blocks, gains, rel_bias):
    rows, heads_dev = gains.shape[1], rel_bias.shape[1]
    extra = jnp.concatenate([gains.T, jnp.pad(rel_bias, ((0, rows - rel_bias.shape[0]), (0, 0)))], axis=1)
    extra = jnp.pad(extra, ((0, 0), (0, QB - extra.shape[1])))
    local = jnp.concatenate(blocks + [extra], axis=1)
    pair = lax.all_gather(local, "model", axis=0)
    cols = []
    off = 0
    for blk in blocks:
        width = blk.shape[1]
        cols.append(pair[0, :, off:off + width])
        cols.append(pair[1, :, off:off + width])
        off += width
    cols += [pair[0, :, off:off + 3 + heads_dev], pair[1, :, off + 3:off + QB - heads_dev]]
    both = jnp.concatenate(cols, axis=1)
    full = lax.all_gather(both, "data", axis=0, tiled=True)
    return full, full[:, 2 * off:2 * off + 3].T, full[:NUM_BUCKETS, 2 * off + 3:2 * off + 3 + 2 * heads_dev]


def scatter_grads(grad_all, gain_part, bias_part, widths):
    blocks = grad_all.shape[0] // 64
    rep_bias = jnp.tile(jnp.pad(bias_part, ((0, 64 - bias_part.shape[0]), (0, 0))), (blocks, 1))
    extra = jnp.concatenate([gain_part.T, rep_bias], axis=1)
    extra = jnp.pad(extra, ((0, 0), (0, QB - extra.shape[1])))
    heads_dev = bias_part.shape[1] // 2
    rows = lax.psum_scatter(jnp.concatenate([grad_all, extra], axis=1), "data", scatter_dimension=0, tiled=True)
    lo, hi = [], []
    off = 0
    for width in widths:
        lo.append(rows[:, off:off + width])
        hi.append(rows[:, off + width:off + 2 * width])
        off += 2 * width
    lo.append(rows[:, off:off + QB])
    hi += [rows[:, off:off + 3], rows[:, off + 3 + heads_dev:off + QB], rows[:, :heads_dev]]
    pair = jnp.stack([jnp.concatenate(lo, axis=1), jnp.concatenate(hi, axis=1)])
    mine = lax.psum_scatter(pair, "model", scatter_dimension=0)
    outs = []
    off = 0
    for width in widths:
        outs.append(mine[:, off:off + width])
        off += width
    return outs, mine[:, off:off + 3], mine[:NUM_BUCKETS, off + 3:off + 3 + heads_dev]


def layer_call(x, e, dy, weights, gains, bias_t):
    steps = x.shape[0] // (2 * SEQS_STEP * SEQ)
    part = lambda rows: pl.BlockSpec((rows, DIM), lambda i: (lax.axis_index("model") * steps + i, 0))
    fixed = lambda arr_shape: pl.BlockSpec(arr_shape, lambda i: (0,) * len(arr_shape), pipeline_mode=pl.Buffered(1))
    anywhere = pl.BlockSpec(memory_space=pl.ANY)
    rows, erows = SEQS_STEP * SEQ, SEQS_STEP * ENC
    seqs = SEQS_STEP * steps
    outs = [jax.ShapeDtypeStruct(x.shape, BF), jax.ShapeDtypeStruct(x.shape, BF), jax.ShapeDtypeStruct(e.shape, BF),
            jax.ShapeDtypeStruct((DIM, C_END), F32), jax.ShapeDtypeStruct((24, DIM), F32), jax.ShapeDtypeStruct((HEADS, SEQ, QB), F32)]
    return pl.pallas_call(
        layer_kernel,
        out_shape=outs,
        grid=(steps,),
        in_specs=[part(rows), part(erows), part(rows), pl.BlockSpec((DIM, C_END), lambda i: (0, 0), pipeline_mode=pl.Buffered(1)), fixed(gains.shape), fixed(bias_t.shape)],
        out_specs=[anywhere, anywhere, anywhere, fixed((DIM, C_END)), fixed((24, DIM)), fixed((HEADS, SEQ, QB))],
        scratch_shapes=[pltpu.VMEM(*item) for item in SCRATCH] + [
            pltpu.VMEM((2, SEQ, DIM), BF), pltpu.VMEM((2, SEQ, DIM), BF), pltpu.VMEM((2, ENC, DIM), BF),
            pltpu.SemaphoreType.DMA((3, 2)), pltpu.SemaphoreType.DMA((3, 2)), pltpu.SemaphoreType.DMA((3, seqs))],
        compiler_params=pltpu.CompilerParams(dimension_semantics=("arbitrary",), vmem_limit_bytes=67043328, collective_id=0, has_side_effects=True),
        name="layer",
    )(x, e, dy, weights, gains, bias_t)


def bias_table():
    dist = (SEQ - QB + jnp.arange(QB))[None, :] - jnp.arange(SEQ)[:, None]
    dist = jnp.maximum(dist, 0)
    edges = jnp.array(BUCKET_EDGES, dtype=jnp.int32)
    ids = jnp.minimum(dist, 16) + jnp.sum((dist[:, :, None] >= edges).astype(jnp.int32), axis=-1)
    return ids


def layer_shard(dec_in, enc_out, grad_out, rel_bias, self_q, self_k, self_v, self_o, cross_q, cross_k, cross_v, cross_o, mlp_wi_0, mlp_wi_1, mlp_wo, norm_self, norm_cross, norm_mlp):
    blocks = pack_local(self_q, self_k, self_v, self_o, cross_q, cross_k, cross_v, cross_o, mlp_wi_0, mlp_wi_1, mlp_wo)
    widths = [blk.shape[1] for blk in blocks]
    weights, gains, bias_pair = gather_weights(blocks, jnp.stack([norm_self, norm_cross, norm_mlp]), rel_bias)
    ids = bias_table()
    hot = (ids[:, :, None] == jnp.arange(NUM_BUCKETS)).astype(F32)
    bias_t = jnp.einsum("car,rh->hca", hot, bias_pair.astype(F32), precision=lax.Precision.HIGHEST)

    def flat(arr):
        return arr.reshape(-1, DIM)

    dec_out, grad_dec, grad_enc, grad_all, gain_part, bias_rows = layer_call(flat(dec_in), flat(enc_out), flat(grad_out), weights, gains.astype(F32), bias_t)
    bias_part = jnp.einsum("car,hca->rh", hot, bias_rows, precision=lax.Precision.HIGHEST)
    gain_part = jnp.sum(gain_part.reshape(3, 8, DIM), axis=1)
    grads, d_gains, grad_bias = scatter_grads(grad_all, gain_part, bias_part, widths)
    o_sq, o_sk, o_sv, o_so, o_cq, o_ck, o_cv, o_co, o_i0, o_i1, o_wo = grads
    return (dec_out.reshape(dec_in.shape), grad_dec.reshape(dec_in.shape), grad_enc.reshape(enc_out.shape), grad_bias, o_sq, o_sk, o_sv, o_so.T, o_cq, o_ck, o_cv, o_co.T, o_i0, o_i1, o_wo.T, d_gains[:, 0], d_gains[:, 1], d_gains[:, 2])


def solution(mesh):
    row_spec = P("data", None, None)
    col_in = P("data", "model")
    col_out = P("model", "data")
    gain_spec = P("data")
    bias_spec = P(None, "model")
    arg_specs = (row_spec, row_spec, row_spec, bias_spec, col_in, col_in, col_in, col_out, col_in, col_in, col_in, col_out, col_in, col_in, col_out, gain_spec, gain_spec, gain_spec)
    out_specs = (row_spec, row_spec, row_spec) + arg_specs[3:]
    return jax.shard_map(layer_shard, mesh=mesh, in_specs=arg_specs, out_specs=out_specs, check_vma=False)
```

```python
import math
import jax
import jax.numpy as jnp
from jax import lax
from jax.experimental import pallas as pl
from jax.experimental.pallas import tpu as pltpu
from jax.sharding import PartitionSpec as P

EPS = 1e-6
NUM_BUCKETS = 32
MASK_VALUE = -1e9
BUCKET_EDGES = tuple(math.ceil(16 * 8.0 ** (bucket_no / 16.0)) for bucket_no in range(1, 16))


SEQ = 384
ENC = 192
DIM = 512
INNER = 384
FF = 1024
HEADS = 6
PAIRS = 3
QB = 128
CHUNK = 64
SEQS_STEP = 2
C_SQ, C_SO, C_CQ, C_CK, C_CO, C_I0, C_I1, C_WO, C_END = 0, 1152, 1536, 1920, 2688, 3072, 4096, 5120, 6144
BF = jnp.bfloat16
F32 = jnp.float32
GELU_C = math.sqrt(2.0 / math.pi)
GELU_K = 0.044715
MESH = pl.DeviceIdType.MESH


def nn(a, b):
    return lax.dot_general(a, b, (((1,), (0,)), ((), ())), preferred_element_type=F32)


def nt(a, b):
    return lax.dot_general(a, b, (((1,), (1,)), ((), ())), preferred_element_type=F32)


def tn(a, b):
    return lax.dot_general(a, b, (((0,), (0,)), ((), ())), preferred_element_type=F32)


def unit_of(act_f):
    inv = lax.rsqrt(jnp.mean(act_f * act_f, axis=-1, keepdims=True) + EPS)
    return act_f * inv, inv


def head_mask(value, head, lane_idx):
    keep = (lane_idx < 64) if head == 0 else (lane_idx >= 64)
    return jnp.where(keep, value.astype(F32), 0.0).astype(BF)


def softmax_t(logits):
    top = jnp.max(logits, axis=0, keepdims=True)
    expd = jnp.exp(logits - top)
    return expd * (1.0 / jnp.sum(expd, axis=0, keepdims=True))


def seq_body(s, exchange, x_ref, e_ref, dy_ref, w_ref, gain_ref, bias_ref, y_buf, dx_buf, de_buf, dg_ref, db_ref,
             n1_s, n2_s, n3_s, dm1_s, dm2_s, qkv_s, dqkv_s, ctx_s, cq_s, ckv_s, dcq_s, dckv_s, cctx_s,
             hid_s, d01_s, x1_s, x2_s, dctx_s, pf_s, pt_s, cpf_s, cpt_s, ds_s, cds_s, km_s, vm_s):
    r0 = pl.multiple_of(s * SEQ, SEQ)
    e0 = pl.multiple_of(s * ENC, ENC)
    rows = pl.ds(r0, SEQ)
    erows = pl.ds(e0, ENC)

    def chunk_rows(off):
        return pl.ds(pl.multiple_of(r0 + off, CHUNK), CHUNK)

    chunks = range(0, SEQ, CHUNK)
    slot, wait_slot, send, weights_here = exchange
    lane_idx = lax.broadcasted_iota(jnp.int32, (SEQ, QB), 1)
    tri = lax.broadcasted_iota(jnp.int32, (QB, QB), 0) <= lax.broadcasted_iota(jnp.int32, (QB, QB), 1)

    for off in chunks:
        unit, _ = unit_of(x_ref[chunk_rows(off), :].astype(F32))
        n1_s[chunk_rows(off), :] = (unit * gain_ref[0:1, :]).astype(BF)
    for col in range(0, 3 * INNER, INNER):
        qkv_s[:, col:col + INNER] = nn(n1_s[rows, :], w_ref[:, C_SQ + col:C_SQ + col + INNER]).astype(BF)

    def self_pair(hp, carry):
        o = pl.multiple_of(hp * QB, QB)
        k_pair = qkv_s[:, pl.ds(pl.multiple_of(INNER + o, QB), QB)]
        v_pair = qkv_s[:, pl.ds(pl.multiple_of(2 * INNER + o, QB), QB)]
        for head in range(2):
            km_s[head * SEQ:(head + 1) * SEQ, :] = head_mask(k_pair, head, lane_idx)
            vm_s[head * SEQ:(head + 1) * SEQ, :] = head_mask(v_pair, head, lane_idx)
        for head in range(2):
            for qb in range(3):
                n = QB * (qb + 1)
                logits = nt(km_s[head * SEQ:head * SEQ + n, :], qkv_s[qb * QB:(qb + 1) * QB, pl.ds(o, QB)])
                logits = logits.astype(BF).astype(F32) + bias_ref[2 * hp + head, SEQ - n:SEQ, :]
                diag = jnp.where(tri, logits[n - QB:n], MASK_VALUE)
                logits = diag if qb == 0 else jnp.concatenate([logits[:n - QB], diag], axis=0)
                probs = softmax_t(logits)
                pf_s[2 * hp + head, 0:n, qb * QB:(qb + 1) * QB] = probs
                pt_s[hp, head * SEQ:head * SEQ + n, qb * QB:(qb + 1) * QB] = probs.astype(BF)
        ctx_s[rows, pl.ds(o, QB)] = tn(pt_s[hp], vm_s[...]).astype(BF)
        return carry

    lax.fori_loop(0, PAIRS, self_pair, 0)

    weights_here(1)

    delta = nt(ctx_s[rows, :], w_ref[:, C_SO:C_SO + INNER])
    for off in chunks:
        mid = (x_ref[chunk_rows(off), :].astype(F32) + delta[off:off + CHUNK]).astype(BF)
        x1_s[off:off + CHUNK, :] = mid
        unit, _ = unit_of(mid.astype(F32))
        n2_s[chunk_rows(off), :] = (unit * gain_ref[1:2, :]).astype(BF)
    cq_s[...] = nn(n2_s[rows, :], w_ref[:, C_CQ:C_CQ + INNER]).astype(BF)
    ckv_s[...] = nn(e_ref[erows, :], w_ref[:, C_CK:C_CK + 2 * INNER]).astype(BF)

    def cross_masks(o):
        k_pair = ckv_s[:, pl.ds(o, QB)]
        v_pair = ckv_s[:, pl.ds(pl.multiple_of(INNER + o, QB), QB)]
        for head in range(2):
            km_s[head * ENC:(head + 1) * ENC, :] = head_mask(k_pair, head, lane_idx[:ENC])
            vm_s[head * ENC:(head + 1) * ENC, :] = head_mask(v_pair, head, lane_idx[:ENC])

    def cross_pair(hp, carry):
        o = pl.multiple_of(hp * QB, QB)
        cross_masks(o)
        for head in range(2):
            for qb in range(3):
                cols = slice(qb * QB, (qb + 1) * QB)
                logits = nt(km_s[head * ENC:(head + 1) * ENC, :], cq_s[cols, pl.ds(o, QB)])
                probs = softmax_t(logits.astype(BF).astype(F32))
                cpf_s[2 * hp + head, :, cols] = probs
                cpt_s[hp, head * ENC:(head + 1) * ENC, cols] = probs.astype(BF)
        cctx_s[rows, pl.ds(o, QB)] = tn(cpt_s[hp], vm_s[0:2 * ENC, :]).astype(BF)
        return carry

    lax.fori_loop(0, PAIRS, cross_pair, 0)

    weights_here(2)

    delta = nt(cctx_s[rows, :], w_ref[:, C_CO:C_CO + INNER])
    for off in chunks:
        mid = (x1_s[off:off + CHUNK, :].astype(F32) + delta[off:off + CHUNK]).astype(BF)
        x2_s[off:off + CHUNK, :] = mid
        unit, _ = unit_of(mid.astype(F32))
        n3_s[chunk_rows(off), :] = (unit * gain_ref[2:3, :]).astype(BF)
    step = 256
    for col in range(0, FF, step):
        pre_0 = nn(n3_s[rows, :], w_ref[:, C_I0 + col:C_I0 + col + step])
        pre_1 = nn(n3_s[rows, :], w_ref[:, C_I1 + col:C_I1 + col + step])
        d_hid = nn(dy_ref[rows, :], w_ref[:, C_WO + col:C_WO + col + step])
        for off in chunks:
            a0 = pre_0[off:off + CHUNK].astype(BF).astype(F32)
            a1 = pre_1[off:off + CHUNK].astype(BF).astype(F32)
            dh = d_hid[off:off + CHUNK].astype(BF).astype(F32)
            sq = a0 * a0
            half = 0.5 * jnp.tanh(a0 * (GELU_C + (GELU_C * GELU_K) * sq)) + 0.5
            gelu = a0 * half
            slope = half * (1.0 + (a0 - gelu) * (2.0 * GELU_C + (6.0 * GELU_C * GELU_K) * sq))
            hid_s[chunk_rows(off), col:col + step] = (gelu * a1).astype(BF)
            d01_s[chunk_rows(off), col:col + step] = (slope * (dh * a1)).astype(BF)
            d01_s[chunk_rows(off), FF + col:FF + col + step] = (dh * gelu).astype(BF)
    delta = nt(hid_s[rows, :], w_ref[:, C_WO:C_WO + FF])
    wait_slot(0)
    for off in chunks:
        y_buf[slot, off:off + CHUNK, :] = (x2_s[off:off + CHUNK, :].astype(F32) + delta[off:off + CHUNK]).astype(BF)
    send(0)

    def norm_back(d_norm, base, d_res, out, idx):
        total = dg_ref[8 * idx:8 * idx + 8, :]
        for off in chunks:
            d_n = d_norm[off:off + CHUNK].astype(BF).astype(F32)
            unit, inv = unit_of(base(off).astype(F32))
            total = total + jnp.sum((d_n * unit).reshape(CHUNK // 8, 8, DIM), axis=0)
            d_unit = d_n * gain_ref[idx:idx + 1, :]
            d_act = inv * (d_unit - unit * jnp.mean(d_unit * unit, axis=-1, keepdims=True))
            out(off)[...] = (d_res[chunk_rows(off), :].astype(F32) + d_act).astype(BF)
        dg_ref[8 * idx:8 * idx + 8, :] = total

    d_norm = nt(d01_s[rows, :], w_ref[:, C_I0:C_I0 + 2 * FF])
    norm_back(d_norm, lambda off: x2_s[off:off + CHUNK, :], dy_ref, lambda off: dm2_s.at[chunk_rows(off), :], 2)

    dctx_s[...] = nn(dm2_s[rows, :], w_ref[:, C_CO:C_CO + INNER]).astype(BF)

    def cross_pair_back(hp, carry):
        o = pl.multiple_of(hp * QB, QB)
        cross_masks(o)
        for head in range(2):
            for qb in range(3):
                cols = slice(qb * QB, (qb + 1) * QB)
                d_p = nt(vm_s[head * ENC:(head + 1) * ENC, :], dctx_s[cols, pl.ds(o, QB)]).astype(BF).astype(F32)
                probs = cpf_s[2 * hp + head, :, cols]
                d_l = probs * (d_p - jnp.sum(probs * d_p, axis=0, keepdims=True))
                cds_s[head * ENC:(head + 1) * ENC, cols] = d_l.astype(BF)
        dcq_s[rows, pl.ds(o, QB)] = tn(cds_s[...], km_s[0:2 * ENC, :]).astype(BF)
        d_k = nn(cds_s[...], cq_s[:, pl.ds(o, QB)])
        d_v = nn(cpt_s[hp], dctx_s[:, pl.ds(o, QB)])
        low = lane_idx[:ENC] < 64
        dckv_s[erows, pl.ds(o, QB)] = jnp.where(low, d_k[:ENC], d_k[ENC:]).astype(BF)
        dckv_s[erows, pl.ds(pl.multiple_of(INNER + o, QB), QB)] = jnp.where(low, d_v[:ENC], d_v[ENC:]).astype(BF)
        return carry

    lax.fori_loop(0, PAIRS, cross_pair_back, 0)
    d_norm = nt(dcq_s[rows, :], w_ref[:, C_CQ:C_CQ + INNER])
    wait_slot(2)
    de_buf[slot] = nt(dckv_s[erows, :], w_ref[:, C_CK:C_CK + 2 * INNER]).astype(BF)
    send(2)
    norm_back(d_norm, lambda off: x1_s[off:off + CHUNK, :], dm2_s, lambda off: dm1_s.at[chunk_rows(off), :], 1)

    dctx_s[...] = nn(dm1_s[rows, :], w_ref[:, C_SO:C_SO + INNER]).astype(BF)

    def self_pair_back(hp, carry):
        o = pl.multiple_of(hp * QB, QB)
        k_pair = qkv_s[:, pl.ds(pl.multiple_of(INNER + o, QB), QB)]
        v_pair = qkv_s[:, pl.ds(pl.multiple_of(2 * INNER + o, QB), QB)]
        for head in range(2):
            km_s[head * SEQ:(head + 1) * SEQ, :] = head_mask(k_pair, head, lane_idx)
            vm_s[head * SEQ:(head + 1) * SEQ, :] = head_mask(v_pair, head, lane_idx)
        for head in range(2):
            for qb in range(3):
                n = QB * (qb + 1)
                cols = slice(qb * QB, (qb + 1) * QB)
                d_p = nt(vm_s[head * SEQ:head * SEQ + n, :], dctx_s[cols, pl.ds(o, QB)]).astype(BF).astype(F32)
                probs = pf_s[2 * hp + head, 0:n, cols]
                d_l = probs * (d_p - jnp.sum(probs * d_p, axis=0, keepdims=True))
                db_ref[2 * hp + head, SEQ - n:SEQ, :] += d_l
                ds_s[head * SEQ:head * SEQ + n, cols] = d_l.astype(BF)
        dqkv_s[rows, pl.ds(o, QB)] = tn(ds_s[...], km_s[...]).astype(BF)
        d_k = nn(ds_s[...], qkv_s[:, pl.ds(o, QB)])
        d_v = nn(pt_s[hp], dctx_s[:, pl.ds(o, QB)])
        low = lane_idx < 64
        dqkv_s[rows, pl.ds(pl.multiple_of(INNER + o, QB), QB)] = jnp.where(low, d_k[:SEQ], d_k[SEQ:]).astype(BF)
        dqkv_s[rows, pl.ds(pl.multiple_of(2 * INNER + o, QB), QB)] = jnp.where(low, d_v[:SEQ], d_v[SEQ:]).astype(BF)
        return carry

    lax.fori_loop(0, PAIRS, self_pair_back, 0)
    d_norm = nt(dqkv_s[rows, :], w_ref[:, C_SQ:C_SQ + 3 * INNER])
    wait_slot(1)
    norm_back(d_norm, lambda off: x_ref[chunk_rows(off), :], dm1_s, lambda off: dx_buf.at[slot, off:off + CHUNK, :], 0)
    send(1)


SCRATCH = [
    ((2 * SEQ, DIM), BF),
    ((2 * SEQ, DIM), BF),
    ((2 * SEQ, DIM), BF),
    ((2 * SEQ, DIM), BF),
    ((2 * SEQ, DIM), BF),
    ((SEQ, 3 * INNER), BF),
    ((2 * SEQ, 3 * INNER), BF),
    ((2 * SEQ, INNER), BF),
    ((SEQ, INNER), BF),
    ((ENC, 2 * INNER), BF),
    ((2 * SEQ, INNER), BF),
    ((2 * ENC, 2 * INNER), BF),
    ((2 * SEQ, INNER), BF),
    ((2 * SEQ, FF), BF),
    ((2 * SEQ, 2 * FF), BF),
    ((SEQ, DIM), BF),
    ((SEQ, DIM), BF),
    ((SEQ, INNER), BF),
    ((HEADS, SEQ, SEQ), F32),
    ((PAIRS, 2 * SEQ, SEQ), BF),
    ((HEADS, ENC, SEQ), F32),
    ((PAIRS, 2 * ENC, SEQ), BF),
    ((2 * SEQ, SEQ), BF),
    ((2 * ENC, SEQ), BF),
    ((2 * SEQ, QB), BF),
    ((2 * SEQ, QB), BF),
]


def weight_grads(g_ref, e_ref, dy_ref, n1_s, n2_s, n3_s, dm1_s, dm2_s, dqkv_s, ctx_s, dcq_s, dckv_s, cctx_s, hid_s, d01_s):
    def add(act, d_out, col, width):
        for off in range(0, width, 384 if width % 384 == 0 else 512):
            size = 384 if width % 384 == 0 else 512
            g_ref[:, col + off:col + off + size] += tn(act[...], d_out[:, off:off + size])

    add(n3_s, d01_s, C_I0, 2 * FF)
    add(dy_ref, hid_s, C_WO, FF)
    add(dm2_s, cctx_s, C_CO, INNER)
    add(n2_s, dcq_s, C_CQ, INNER)
    add(e_ref, dckv_s, C_CK, 2 * INNER)
    add(dm1_s, ctx_s, C_SO, INNER)
    add(n1_s, dqkv_s, C_SQ, 3 * INNER)


O_I0, O_I1, O_WO, O_EX, O_END = 2048, 2560, 3072, 3584, 3712
PACKED = (((0, 1024), (O_EX, QB)), ((1024, 1024),), ((O_I0, 1536),))
WHOLE = (((0, 1536), (C_END, QB)), ((1536, 1536),), ((C_I0, 3072),))
X_FIRST = (((0, 768),), ((1536, 768),), ((C_I0, 1536),))
Y_FIRST = (((768, 768), (C_END, QB)), ((2304, 768),), ((C_I0 + 1536, 1536),))
GATHER_SEMS = 48
THRESHOLDS = tuple(range(1, 17)) + BUCKET_EDGES


def gather_plan(loc_ref, rz_s, w_s, send_sem, recv_sem):
    m, d = lax.axis_index("model"), lax.axis_index("data")
    core, x, y = lax.rem(d, 2), lax.rem(d // 2, 2), d // 4
    d_core, d_x, d_y = d + 1 - 2 * core, d + 2 - 4 * x, d + 4 - 8 * y
    count = [0]

    def copy(src, dst, peer):
        number = count[0]
        count[0] += 1
        return lambda: pltpu.make_async_remote_copy(src_ref=src, dst_ref=dst, send_sem=send_sem.at[number], recv_sem=recv_sem.at[number],
                                                    device_id=peer, device_id_type=MESH)

    def block(owner, run):
        return w_s.at[pl.ds(pl.multiple_of(owner * 64, 64), 64), run[0]:run[0] + run[1]]

    def blocks(owners, runs, peer):
        return [copy(block(owner, run), block(owner, run), peer) for owner in owners for run in runs]

    plan = []
    for group in range(3):
        z = [copy(loc_ref.at[:, a:a + n], rz_s.at[:, a:a + n], {"model": 1 - m}) for a, n in PACKED[group]]
        second = blocks([d], X_FIRST[group], {"data": d_x}) + blocks([d], Y_FIRST[group], {"data": d_y})
        third = blocks([d, d_x], X_FIRST[group], {"data": d_y}) + blocks([d, d_y], Y_FIRST[group], {"data": d_x})
        mine = [core, core + 2, core + 4, core + 6]
        plan.append((z, second, third, blocks(mine, WHOLE[group], {"data": d_core})))
    return plan


def pack_share(attn, mlp, ext_ref, loc_s):
    m = lax.axis_index("model")
    for b, ref in enumerate(attn):
        left = jnp.concatenate([ref[...].astype(F32), jnp.zeros((64, 64), F32)], axis=1)
        loc_s[:, 256 * b:256 * b + 256] = jnp.where(m == 0, left, pltpu.roll(left, 64, 1)).astype(BF)
    for col, ref in zip((O_I0, O_I1, O_WO), mlp):
        loc_s[:, col:col + 512] = ref[...]
    loc_s[:, O_EX:O_END] = ext_ref[...]


def fill_gains(w_s, gain_s):
    low = lax.broadcasted_iota(jnp.int32, (8, QB), 1) < 64
    for pair in range(4):
        even = w_s[128 * pair:128 * pair + 16, C_END:C_END + QB].astype(F32)[0:8]
        odd = w_s[128 * pair + 64:128 * pair + 80, C_END:C_END + QB].astype(F32)[0:8]
        gain_s[:, QB * pair:QB * pair + QB] = jnp.where(low, even, pltpu.roll(odd, 64, 1))


def small_grads(dg_s, db_s, ext_ref):
    dist = jnp.maximum(SEQ - QB + lax.broadcasted_iota(jnp.int32, (SEQ, QB), 1) - lax.broadcasted_iota(jnp.int32, (SEQ, QB), 0), 0)
    ids = jnp.zeros((SEQ, QB), jnp.int32)
    for edge in THRESHOLDS:
        ids = ids + (dist >= edge).astype(jnp.int32)
    lane = lax.broadcasted_iota(jnp.int32, (NUM_BUCKETS, QB), 1)
    row = lax.broadcasted_iota(jnp.int32, (NUM_BUCKETS, QB), 0)
    bias = jnp.zeros((NUM_BUCKETS, QB), F32)
    for head in range(HEADS):
        def bucket_sum(bucket, sums):
            part = jnp.sum(jnp.where(ids == bucket, db_s[head], 0.0), axis=0, keepdims=True)
            return jnp.where(row == bucket, part, sums)
        sums = lax.fori_loop(0, NUM_BUCKETS, bucket_sum, jnp.zeros((NUM_BUCKETS, QB), F32))
        bias = jnp.where(lane == 64 + head, jnp.sum(sums, axis=1, keepdims=True), bias)
    row8 = lax.broadcasted_iota(jnp.int32, (8, DIM), 0)
    gains = jnp.zeros((8, DIM), F32)
    for idx in range(3):
        gains = jnp.where(row8 == idx, jnp.sum(dg_s[8 * idx:8 * idx + 8, :], axis=0, keepdims=True), gains)
    low = lax.broadcasted_iota(jnp.int32, (8, QB), 1) < 64
    for d in range(8):
        tile = gains[:, QB * (d // 2):QB * (d // 2) + QB]
        if d % 2:
            tile = pltpu.roll(tile, 64, 1)
        ext_ref[64 * d:64 * d + 8, :] = jnp.where(low, tile, bias[0:8])
        ext_ref[64 * d + 8:64 * d + NUM_BUCKETS, :] = bias[8:]
        ext_ref[64 * d + NUM_BUCKETS:64 * d + 64, :] = jnp.zeros((32, QB), F32)


def merge_share(group, loc_ref, rz_s, w_s):
    m, d = lax.axis_index("model"), lax.axis_index("data")
    rows = pl.ds(pl.multiple_of(d * 64, 64), 64)

    def both(a, n):
        here, there = loc_ref[:, a:a + n].astype(F32), rz_s[:, a:a + n].astype(F32)
        return jnp.where(m == 0, here, there), jnp.where(m == 0, there, here)

    if group == 2:
        for a, col in ((O_I0, C_I0), (O_I1, C_I1), (O_WO, C_WO)):
            low, high = both(a, 512)
            w_s[rows, col:col + 512] = low.astype(BF)
            w_s[rows, col + 512:col + 1024] = high.astype(BF)
        return
    for b in range(4 * group, 4 * group + 4):
        low, high = both(256 * b, 256)
        w_s[rows, INNER * b:INNER * b + QB] = low[:, :QB].astype(BF)
        w_s[rows, INNER * b + QB:INNER * b + 2 * QB] = (low[:, QB:] + high[:, :QB]).astype(BF)
        w_s[rows, INNER * b + 2 * QB:INNER * b + 3 * QB] = high[:, QB:].astype(BF)
    if group == 0:
        w_s[rows, C_END:C_END + QB] = loc_ref[:, O_EX:O_END]


def begin(copies):
    for make in copies:
        make().start()


def arrive_all(copies):
    for make in copies:
        make().wait_recv()


def fill_bias(loc_ref, rz_s, bias_s):
    m = lax.axis_index("model")
    here, there = loc_ref[0:NUM_BUCKETS, O_EX:O_END].astype(F32), rz_s[0:NUM_BUCKETS, O_EX:O_END].astype(F32)
    tables = jnp.where(m == 0, here, there), jnp.where(m == 0, there, here)
    dist = SEQ - QB + lax.broadcasted_iota(jnp.int32, (SEQ, QB), 1) - lax.broadcasted_iota(jnp.int32, (SEQ, QB), 0)
    for head in range(HEADS):
        table = tables[head // 3]
        lane = 64 + head % 3
        value = jnp.broadcast_to(table[0:1, lane:lane + 1], (SEQ, QB))
        for bucket, edge in enumerate(THRESHOLDS):
            value = jnp.where(dist >= edge, table[bucket + 1:bucket + 2, lane:lane + 1], value)
        bias_s[head] = value


def layer_kernel(x_ref, e_ref, dy_ref, *refs):
    attn, mlp, (extra_ref, y_hbm, dx_hbm, de_hbm, g_ref, ext_ref), scratch = refs[:8], refs[8:11], refs[11:17], refs[17:]
    *scratch, y_buf, dx_buf, de_buf, w_ref, rz_s, gain_ref, bias_ref, loc_ref, dg_ref, db_ref, local_sem, send_sem, recv_sem, w_send, w_recv = scratch
    plan = gather_plan(loc_ref, rz_s, w_ref, w_send, w_recv)
    (n1_s, n2_s, n3_s, dm1_s, dm2_s, qkv_s, dqkv_s, ctx_s, cq_s, ckv_s, dcq_s, dckv_s, cctx_s,
     hid_s, d01_s, x1_s, x2_s, dctx_s, pf_s, pt_s, cpf_s, cpt_s, ds_s, cds_s, km_s, vm_s) = scratch
    me = lax.axis_index("model")
    other = 1 - me
    step = pl.program_id(0)
    seqs = SEQS_STEP * pl.num_programs(0)
    bufs = ((y_buf, y_hbm, SEQ), (dx_buf, dx_hbm, SEQ), (de_buf, de_hbm, ENC))

    @pl.when(step == 0)
    def _():
        d = lax.axis_index("data")
        core, x, y = lax.rem(d, 2), lax.rem(d // 2, 2), d // 4
        barrier = pltpu.get_barrier_semaphore()
        for peer in ({"model": other}, {"data": d + 1 - 2 * core}, {"data": d + 2 - 4 * x}, {"data": d + 4 - 8 * y}):
            pl.semaphore_signal(barrier, inc=1, device_id=peer, device_id_type=MESH)
        pl.semaphore_wait(barrier, 4)
        pack_share(attn, mlp, extra_ref, loc_ref)
        for group in range(3):
            begin(plan[group][0])
        arrive_all(plan[0][0])
        merge_share(0, loc_ref, rz_s, w_ref)
        begin(plan[0][1])
        arrive_all(plan[1][0])
        merge_share(1, loc_ref, rz_s, w_ref)
        begin(plan[1][1])
        arrive_all(plan[0][1])
        begin(plan[0][2])
        arrive_all(plan[2][0])
        merge_share(2, loc_ref, rz_s, w_ref)
        begin(plan[2][1])
        arrive_all(plan[1][1])
        begin(plan[1][2])
        fill_bias(loc_ref, rz_s, bias_ref)
        pt_s[...] = jnp.zeros_like(pt_s)
        ds_s[...] = jnp.zeros_like(ds_s)
        dg_ref[...] = jnp.zeros_like(dg_ref)
        db_ref[...] = jnp.zeros_like(db_ref)
        arrive_all(plan[0][2])
        begin(plan[0][3])
        arrive_all(plan[2][1])
        begin(plan[2][2])
        g_ref[...] = jnp.zeros_like(g_ref)
        arrive_all(plan[0][3])
        fill_gains(w_ref, gain_ref)

    def copies(which, number):
        buf, hbm, length = bufs[which]
        slot = lax.rem(number, 2)
        rows = pl.ds(pl.multiple_of((me * seqs + number) * length, length), length)
        local = pltpu.make_async_copy(buf.at[slot], hbm.at[rows, :], local_sem.at[which, slot])
        remote = pltpu.make_async_remote_copy(
            src_ref=buf.at[slot], dst_ref=hbm.at[rows, :], send_sem=send_sem.at[which, slot],
            recv_sem=recv_sem.at[which, number], device_id={"model": other}, device_id_type=MESH)
        return local, remote

    def body(s, carry):
        number = step * SEQS_STEP + s

        def wait_slot(which):
            @pl.when(number >= 2)
            def _():
                local, remote = copies(which, number - 2)
                local.wait()
                remote.wait_send()

        def send(which):
            local, remote = copies(which, number)
            remote.start()
            local.start()

        def weights_here(group):
            @pl.when(number == 0)
            def _():
                arrive_all(plan[group][2])
                begin(plan[group][3])
                arrive_all(plan[group][3])
                if group == 2:
                    for phases in plan:
                        for phase in phases:
                            for make in phase:
                                make().wait_send()

        seq_body(s, (lax.rem(number, 2), wait_slot, send, weights_here), x_ref, e_ref, dy_ref, w_ref, gain_ref, bias_ref, y_buf, dx_buf, de_buf, dg_ref, db_ref, *scratch)
        return carry

    lax.fori_loop(0, SEQS_STEP, body, 0)
    weight_grads(g_ref, e_ref, dy_ref, n1_s, n2_s, n3_s, dm1_s, dm2_s, dqkv_s, ctx_s, dcq_s, dckv_s, cctx_s, hid_s, d01_s)

    @pl.when(step == pl.num_programs(0) - 1)
    def _():
        small_grads(dg_ref, db_ref, ext_ref)
        for which in range(3):
            for back in (2, 1):
                local, remote = copies(which, seqs - back)
                local.wait()
                remote.wait_send()

            def arrived(number, carry):
                copies(which, number)[1].wait_recv()
                return carry

            lax.fori_loop(0, seqs, arrived, 0)


RUNS = (((0, 1920), (C_END, QB)), ((1920, 1152), (C_WO, FF)), ((C_I0, 2 * FF),))


def z_pieces(group):
    attn = [(INNER * b, QB, 256, 256 * b) for b in range(8)]
    if group == 0:
        return attn[:5] + [(C_END, 0, QB, O_EX)]
    if group == 1:
        return attn[5:] + [(C_WO, 512, 512, O_WO)]
    return [(C_I0, 512, 512, O_I0), (C_I1, 512, 512, O_I1)]


Z_WIDTH = tuple(sum(piece[2] for piece in z_pieces(group)) for group in range(3))
RUN_WIDTH = tuple(sum(run[1] for run in RUNS[group]) for group in range(3))
REDUCE_SCRATCH = [(2, 2, 64, C_END + QB), (2, 2, 64, C_END + QB),
                  (2, 64, RUN_WIDTH[0]), (64, RUN_WIDTH[0]), (64, Z_WIDTH[0]),
                  (2, 64, RUN_WIDTH[1]), (2, 64, Z_WIDTH[1]), (64, Z_WIDTH[1]),
                  (2, 2, 64, Z_WIDTH[2]), (2, 64, Z_WIDTH[2]), (64, Z_WIDTH[2])]
REDUCE_SEMS = 64


def reduce_kernel(g_hbm, ext_hbm, out_ref, acc, first, a1, a2, a3, b1, b2, b3, c1, c2, c3, local_sem, send_sem, recv_sem):
    m, d = lax.axis_index("model"), lax.axis_index("data")
    core, x, y = lax.rem(d, 2), lax.rem(d // 2, 2), d // 4
    to_core, to_x, to_y, to_z = {"data": d + 1 - 2 * core}, {"data": d + 2 - 4 * x}, {"data": d + 4 - 8 * y}, {"model": 1 - m}
    barrier = pltpu.get_barrier_semaphore()
    for peer in (to_core, to_x, to_y, to_z):
        pl.semaphore_signal(barrier, inc=1, device_id=peer, device_id_type=MESH)
    pl.semaphore_wait(barrier, 4)
    sent = []

    def push(src, dst, peer):
        number = len(sent)
        copy = pltpu.make_async_remote_copy(src_ref=src, dst_ref=dst, send_sem=send_sem.at[number], recv_sem=recv_sem.at[number],
                                            device_id=peer, device_id_type=MESH)
        copy.start()
        sent.append(copy)
        return copy

    def cols(piece, who):
        return pl.ds(pl.multiple_of(piece[0] + who * piece[1], QB), piece[2])

    loads, pend = {}, {}
    number = 0
    for group in (2, 0, 1):
        loads[group], pend[group] = [], []
        for col, width in RUNS[group]:
            src = ext_hbm if col == C_END else g_hbm
            src_cols = pl.ds(0 if col == C_END else col, width)
            here = pltpu.make_async_copy(src.at[:, :, core, :, src_cols], acc.at[:, :, :, pl.ds(col, width)], local_sem.at[number])
            number += 1
            pend[group].append(push(src.at[:, :, 1 - core, :, src_cols], first.at[:, :, :, pl.ds(col, width)], to_core))
            here.start()
            loads[group].append(here)

    def run_push(group, src_of, dst, peer):
        off, out = 0, []
        for col, width in RUNS[group]:
            out.append(push(src_of(pl.ds(col, width)), dst.at[..., pl.ds(off, width)], peer))
            off += width
        return out

    def z_push(group, src_of, dst, peer, who):
        off, out = 0, []
        for piece in z_pieces(group):
            out.append(push(src_of(cols(piece, who)), dst.at[..., pl.ds(off, piece[2])], peer))
            off += piece[2]
        return out

    for group in (2, 0, 1):
        for here in loads[group]:
            here.wait()
        for copy in pend[group]:
            copy.wait_recv()
        for col, width in RUNS[group]:
            for yy in range(2):
                for xx in range(2):
                    acc[yy, xx, :, col:col + width] += first[yy, xx, :, col:col + width]
        if group == 0:
            pend[0] = run_push(0, lambda c: acc.at[:, 1 - x, :, c], a1, to_x)
        elif group == 1:
            pend[1] = run_push(1, lambda c: acc.at[1 - y, :, :, c], b1, to_y)
        else:
            pend[2] = z_push(2, lambda c: acc.at[:, :, :, c], c1, to_z, 1 - m)

    def arrive(group):
        for copy in pend[group]:
            copy.wait_recv()

    arrive(0)
    off = 0
    for col, width in RUNS[0]:
        for yy in range(2):
            acc[yy, x, :, col:col + width] += a1[yy, :, off:off + width]
        off += width
    pend[0] = run_push(0, lambda c: acc.at[1 - y, x, :, c], a2, to_y)
    arrive(1)
    off = 0
    for col, width in RUNS[1]:
        for xx in range(2):
            acc[y, xx, :, col:col + width] += b1[xx, :, off:off + width]
        off += width
    pend[1] = z_push(1, lambda c: acc.at[y, :, :, c], b2, to_z, 1 - m)
    arrive(2)
    off = 0
    for piece in z_pieces(2):
        for yy in range(2):
            for xx in range(2):
                acc[yy, xx, :, cols(piece, m)] += c1[yy, xx, :, off:off + piece[2]]
        off += piece[2]
    pend[2] = z_push(2, lambda c: acc.at[:, 1 - x, :, c], c2, to_x, m)

    arrive(0)
    off = 0
    for col, width in RUNS[0]:
        acc[y, x, :, col:col + width] += a2[:, off:off + width]
        off += width
    pend[0] = z_push(0, lambda c: acc.at[y, x, :, c], a3, to_z, 1 - m)
    held = pend[1]
    for copy in held:
        copy.wait_recv()
        copy.wait_send()
    off = 0
    for piece in z_pieces(1):
        for xx in range(2):
            acc[y, xx, :, cols(piece, m)] += b2[xx, :, off:off + piece[2]]
        off += piece[2]
    pend[1] = z_push(1, lambda c: acc.at[y, 1 - x, :, c], b3, to_x, m)
    arrive(2)
    off = 0
    for piece in z_pieces(2):
        for yy in range(2):
            acc[yy, x, :, cols(piece, m)] += c2[yy, :, off:off + piece[2]]
        off += piece[2]
    pend[2] = z_push(2, lambda c: acc.at[1 - y, x, :, c], c3, to_y, m)

    for group, last in ((0, a3), (1, b3), (2, c3)):
        arrive(group)
        off = 0
        for piece in z_pieces(group):
            out_ref[:, piece[3]:piece[3] + piece[2]] = acc[y, x, :, cols(piece, m)] + last[:, off:off + piece[2]]
            off += piece[2]
    for copy in sent:
        if not any(copy is other for other in held):
            copy.wait_send()


def scatter_grads(grad_all, ext):
    m = lax.axis_index("model")
    mine = pl.pallas_call(
        reduce_kernel,
        out_shape=jax.ShapeDtypeStruct((64, O_END), F32),
        in_specs=[pl.BlockSpec(memory_space=pl.ANY)] * 2,
        out_specs=pl.BlockSpec(memory_space=pltpu.VMEM),
        scratch_shapes=[pltpu.VMEM(item, F32) for item in REDUCE_SCRATCH] + [
            pltpu.SemaphoreType.DMA((8,)), pltpu.SemaphoreType.DMA((REDUCE_SEMS,)), pltpu.SemaphoreType.DMA((REDUCE_SEMS,))],
        compiler_params=pltpu.CompilerParams(vmem_limit_bytes=67043328, collective_id=1, has_side_effects=True),
        name="reduce",
    )(grad_all.reshape(2, 2, 2, 64, C_END), ext.reshape(2, 2, 2, 64, QB))
    outs = [jnp.where(m == 0, mine[:, 256 * b:256 * b + 192], mine[:, 256 * b + 64:256 * b + 256]) for b in range(8)]
    outs += [mine[:, O_I0:O_I1], mine[:, O_I1:O_WO], mine[:, O_WO:O_EX]]
    bias = jnp.where(m == 0, mine[:NUM_BUCKETS, O_EX + 64:O_EX + 67], mine[:NUM_BUCKETS, O_EX + 67:O_EX + 70])
    return outs, mine[0:3, O_EX:O_EX + 64], bias


def layer_call(x, e, dy, attn, mlp, extra):
    steps = x.shape[0] // (2 * SEQS_STEP * SEQ)
    part = lambda rows: pl.BlockSpec((rows, DIM), lambda i: (lax.axis_index("model") * steps + i, 0))
    fixed = lambda arr_shape: pl.BlockSpec(arr_shape, lambda i: (0,) * len(arr_shape), pipeline_mode=pl.Buffered(1))
    anywhere = pl.BlockSpec(memory_space=pl.ANY)
    rows, erows = SEQS_STEP * SEQ, SEQS_STEP * ENC
    seqs = SEQS_STEP * steps
    outs = [jax.ShapeDtypeStruct(x.shape, BF), jax.ShapeDtypeStruct(x.shape, BF), jax.ShapeDtypeStruct(e.shape, BF),
            jax.ShapeDtypeStruct((DIM, C_END), F32), jax.ShapeDtypeStruct((DIM, QB), F32)]
    return pl.pallas_call(
        layer_kernel,
        out_shape=outs,
        grid=(steps,),
        in_specs=[part(rows), part(erows), part(rows)] + [fixed(w.shape) for w in attn + mlp + [extra]],
        out_specs=[anywhere, anywhere, anywhere, fixed((DIM, C_END)), fixed((DIM, QB))],
        scratch_shapes=[pltpu.VMEM(*item) for item in SCRATCH] + [
            pltpu.VMEM((2, SEQ, DIM), BF), pltpu.VMEM((2, SEQ, DIM), BF), pltpu.VMEM((2, ENC, DIM), BF),
            pltpu.VMEM((DIM, C_END + QB), BF), pltpu.VMEM((64, O_END), BF), pltpu.VMEM((8, DIM), F32), pltpu.VMEM((HEADS, SEQ, QB), F32),
            pltpu.VMEM((64, O_END), BF), pltpu.VMEM((24, DIM), F32), pltpu.VMEM((HEADS, SEQ, QB), F32),
            pltpu.SemaphoreType.DMA((3, 2)), pltpu.SemaphoreType.DMA((3, 2)), pltpu.SemaphoreType.DMA((3, seqs)),
            pltpu.SemaphoreType.DMA((GATHER_SEMS,)), pltpu.SemaphoreType.DMA((GATHER_SEMS,))],
        compiler_params=pltpu.CompilerParams(dimension_semantics=("arbitrary",), vmem_limit_bytes=67043328, collective_id=0, has_side_effects=True),
        name="layer",
    )(x, e, dy, *attn, *mlp, extra)


def layer_shard(dec_in, enc_out, grad_out, rel_bias, self_q, self_k, self_v, self_o, cross_q, cross_k, cross_v, cross_o, mlp_wi_0, mlp_wi_1, mlp_wo, norm_self, norm_cross, norm_mlp):
    gains = jnp.stack([norm_self, norm_cross, norm_mlp])
    extra = jnp.pad(gains, ((0, 61), (0, 64))) + jnp.pad(rel_bias, ((0, 32), (64, 61)))

    def flat(arr):
        return arr.reshape(-1, DIM)

    attn = [self_q, self_k, self_v, self_o.T, cross_q, cross_k, cross_v, cross_o.T]
    dec_out, grad_dec, grad_enc, grad_all, grad_ext = layer_call(flat(dec_in), flat(enc_out), flat(grad_out), attn, [mlp_wi_0, mlp_wi_1, mlp_wo.T], extra)
    grads, d_gains, grad_bias = scatter_grads(grad_all, grad_ext)
    o_sq, o_sk, o_sv, o_so, o_cq, o_ck, o_cv, o_co, o_i0, o_i1, o_wo = grads
    return (dec_out.reshape(dec_in.shape), grad_dec.reshape(dec_in.shape), grad_enc.reshape(enc_out.shape), grad_bias, o_sq, o_sk, o_sv, o_so.T, o_cq, o_ck, o_cv, o_co.T, o_i0, o_i1, o_wo.T, d_gains[0], d_gains[1], d_gains[2])


def solution(mesh):
    row_spec = P("data", None, None)
    col_in = P("data", "model")
    col_out = P("model", "data")
    gain_spec = P("data")
    bias_spec = P(None, "model")
    arg_specs = (row_spec, row_spec, row_spec, bias_spec, col_in, col_in, col_in, col_out, col_in, col_in, col_in, col_out, col_in, col_in, col_out, gain_spec, gain_spec, gain_spec)
    out_specs = (row_spec, row_spec, row_spec) + arg_specs[3:]
    return jax.shard_map(layer_shard, mesh=mesh, in_specs=arg_specs, out_specs=out_specs, check_vma=False)
```

```python
import itertools
import math
import jax
import jax.numpy as jnp
from jax import lax
from jax.experimental import pallas as pl
from jax.experimental.pallas import tpu as pltpu
from jax.sharding import PartitionSpec as P

EPS = 1e-6
NUM_BUCKETS = 32
MASK_VALUE = -1e9
BUCKET_EDGES = tuple(math.ceil(16 * 8.0 ** (bucket_no / 16.0)) for bucket_no in range(1, 16))


SEQ = 384
ENC = 192
DIM = 512
INNER = 384
FF = 1024
HEADS = 6
PAIRS = 3
QB = 128
CHUNK = 64
MLP_ROWS = 192
SEQS_STEP = 2
C_SQ, C_SO, C_CQ, C_CK, C_CO, C_I0, C_I1, C_WO, C_END = 0, 1152, 1536, 1920, 2688, 3072, 4096, 5120, 6144
BF = jnp.bfloat16
F32 = jnp.float32
GELU_C = math.sqrt(2.0 / math.pi)
GELU_K = 0.044715
MESH = pl.DeviceIdType.MESH


def nn(a, b):
    return lax.dot_general(a, b, (((1,), (0,)), ((), ())), preferred_element_type=F32)


def nt(a, b):
    return lax.dot_general(a, b, (((1,), (1,)), ((), ())), preferred_element_type=F32)


def tn(a, b):
    return lax.dot_general(a, b, (((0,), (0,)), ((), ())), preferred_element_type=F32)


def unit_of(act_f):
    inv = lax.rsqrt(jnp.mean(act_f * act_f, axis=-1, keepdims=True) + EPS)
    return act_f * inv, inv


def head_mask(value, head, lane_idx):
    keep = (lane_idx < 64) if head == 0 else (lane_idx >= 64)
    return jnp.where(keep, value.astype(F32), 0.0).astype(BF)


def softmax_t(logits):
    top = jnp.max(logits, axis=0, keepdims=True)
    expd = jnp.exp(logits - top)
    return expd * (1.0 / jnp.sum(expd, axis=0, keepdims=True))


def seq_body(s, exchange, x_ref, e_ref, dy_ref, w_ref, gain_ref, bias_ref, y_buf, dx_buf, de_buf, dg_ref, db_ref,
             n1_s, n2_s, n3_s, dm1_s, dm2_s, qkv_s, dqkv_s, ctx_s, cq_s, ckv_s, dcq_s, dckv_s, cctx_s,
             hid_s, d01_s, x1_s, x2_s, dctx_s, pf_s, pt_s, cpf_s, cpt_s, ds_s, cds_s, km_s, vm_s):
    r0 = pl.multiple_of(s * SEQ, SEQ)
    e0 = pl.multiple_of(s * ENC, ENC)
    rows = pl.ds(r0, SEQ)
    erows = pl.ds(e0, ENC)

    def chunk_rows(off):
        return pl.ds(pl.multiple_of(r0 + off, CHUNK), CHUNK)

    chunks = range(0, SEQ, CHUNK)
    slot, wait_slot, send, weights_here, tail = exchange
    lane_idx = lax.broadcasted_iota(jnp.int32, (SEQ, QB), 1)
    tri = lax.broadcasted_iota(jnp.int32, (QB, QB), 0) <= lax.broadcasted_iota(jnp.int32, (QB, QB), 1)

    for off in chunks:
        unit, _ = unit_of(x_ref[chunk_rows(off), :].astype(F32))
        n1_s[chunk_rows(off), :] = (unit * gain_ref[0:1, :]).astype(BF)
    for col in range(0, 3 * INNER, INNER):
        qkv_s[:, col:col + INNER] = nn(n1_s[rows, :], w_ref[:, C_SQ + col:C_SQ + col + INNER]).astype(BF)

    def self_pair(hp, carry):
        o = pl.multiple_of(hp * QB, QB)
        k_pair = qkv_s[:, pl.ds(pl.multiple_of(INNER + o, QB), QB)]
        v_pair = qkv_s[:, pl.ds(pl.multiple_of(2 * INNER + o, QB), QB)]
        for head in range(2):
            km_s[head * SEQ:(head + 1) * SEQ, :] = head_mask(k_pair, head, lane_idx)
            vm_s[head * SEQ:(head + 1) * SEQ, :] = head_mask(v_pair, head, lane_idx)
        for head in range(2):
            for qb in range(3):
                n = QB * (qb + 1)
                logits = nt(km_s[head * SEQ:head * SEQ + n, :], qkv_s[qb * QB:(qb + 1) * QB, pl.ds(o, QB)])
                logits = logits.astype(BF).astype(F32) + bias_ref[2 * hp + head, SEQ - n:SEQ, :]
                diag = jnp.where(tri, logits[n - QB:n], MASK_VALUE)
                logits = diag if qb == 0 else jnp.concatenate([logits[:n - QB], diag], axis=0)
                probs = softmax_t(logits)
                pf_s[2 * hp + head, 0:n, qb * QB:(qb + 1) * QB] = probs
                pt_s[hp, head * SEQ:head * SEQ + n, qb * QB:(qb + 1) * QB] = probs.astype(BF)
        ctx_s[rows, pl.ds(o, QB)] = tn(pt_s[hp], vm_s[...]).astype(BF)
        return carry

    lax.fori_loop(0, PAIRS, self_pair, 0)

    weights_here(1)

    delta = nt(ctx_s[rows, :], w_ref[:, C_SO:C_SO + INNER])
    for off in chunks:
        mid = (x_ref[chunk_rows(off), :].astype(F32) + delta[off:off + CHUNK]).astype(BF)
        x1_s[off:off + CHUNK, :] = mid
        unit, _ = unit_of(mid.astype(F32))
        n2_s[chunk_rows(off), :] = (unit * gain_ref[1:2, :]).astype(BF)
    cq_s[...] = nn(n2_s[rows, :], w_ref[:, C_CQ:C_CQ + INNER]).astype(BF)
    ckv_s[...] = nn(e_ref[erows, :], w_ref[:, C_CK:C_CK + 2 * INNER]).astype(BF)

    def cross_masks(o):
        k_pair = ckv_s[:, pl.ds(o, QB)]
        v_pair = ckv_s[:, pl.ds(pl.multiple_of(INNER + o, QB), QB)]
        for head in range(2):
            km_s[head * ENC:(head + 1) * ENC, :] = head_mask(k_pair, head, lane_idx[:ENC])
            vm_s[head * ENC:(head + 1) * ENC, :] = head_mask(v_pair, head, lane_idx[:ENC])

    def cross_pair(hp, carry):
        o = pl.multiple_of(hp * QB, QB)
        cross_masks(o)
        for head in range(2):
            for qb in range(3):
                cols = slice(qb * QB, (qb + 1) * QB)
                logits = nt(km_s[head * ENC:(head + 1) * ENC, :], cq_s[cols, pl.ds(o, QB)])
                probs = softmax_t(logits.astype(BF).astype(F32))
                cpf_s[2 * hp + head, :, cols] = probs
                cpt_s[hp, head * ENC:(head + 1) * ENC, cols] = probs.astype(BF)
        cctx_s[rows, pl.ds(o, QB)] = tn(cpt_s[hp], vm_s[0:2 * ENC, :]).astype(BF)
        return carry

    lax.fori_loop(0, PAIRS, cross_pair, 0)

    weights_here(2)

    delta = nt(cctx_s[rows, :], w_ref[:, C_CO:C_CO + INNER])
    for off in chunks:
        mid = (x1_s[off:off + CHUNK, :].astype(F32) + delta[off:off + CHUNK]).astype(BF)
        x2_s[off:off + CHUNK, :] = mid
        unit, _ = unit_of(mid.astype(F32))
        n3_s[chunk_rows(off), :] = (unit * gain_ref[2:3, :]).astype(BF)
    step = 256
    for col, top in itertools.product(range(0, FF, step), range(0, SEQ, MLP_ROWS)):
        part = pl.ds(pl.multiple_of(r0 + top, CHUNK), MLP_ROWS)
        pre_0 = nn(n3_s[part, :], w_ref[:, C_I0 + col:C_I0 + col + step])
        pre_1 = nn(n3_s[part, :], w_ref[:, C_I1 + col:C_I1 + col + step])
        d_hid = nn(dy_ref[part, :], w_ref[:, C_WO + col:C_WO + col + step])
        for off in range(top, top + MLP_ROWS, CHUNK):
            a0 = pre_0[off - top:off - top + CHUNK].astype(BF).astype(F32)
            a1 = pre_1[off - top:off - top + CHUNK].astype(BF).astype(F32)
            dh = d_hid[off - top:off - top + CHUNK].astype(BF).astype(F32)
            sq = a0 * a0
            half = 0.5 * jnp.tanh(a0 * (GELU_C + (GELU_C * GELU_K) * sq)) + 0.5
            gelu = a0 * half
            slope = half * (1.0 + (a0 - gelu) * (2.0 * GELU_C + (6.0 * GELU_C * GELU_K) * sq))
            hid_s[chunk_rows(off), col:col + step] = (gelu * a1).astype(BF)
            d01_s[chunk_rows(off), col:col + step] = (slope * (dh * a1)).astype(BF)
            d01_s[chunk_rows(off), FF + col:FF + col + step] = (dh * gelu).astype(BF)
    delta = nt(hid_s[rows, :], w_ref[:, C_WO:C_WO + FF])
    wait_slot(0)
    for off in chunks:
        y_buf[slot, off:off + CHUNK, :] = (x2_s[off:off + CHUNK, :].astype(F32) + delta[off:off + CHUNK]).astype(BF)
    send(0)

    def norm_back(d_norm, base, d_res, out, idx):
        total = dg_ref[8 * idx:8 * idx + 8, :]
        for off in chunks:
            d_n = d_norm[off:off + CHUNK].astype(BF).astype(F32)
            unit, inv = unit_of(base(off).astype(F32))
            total = total + jnp.sum((d_n * unit).reshape(CHUNK // 8, 8, DIM), axis=0)
            d_unit = d_n * gain_ref[idx:idx + 1, :]
            d_act = inv * (d_unit - unit * jnp.mean(d_unit * unit, axis=-1, keepdims=True))
            out(off)[...] = (d_res[chunk_rows(off), :].astype(F32) + d_act).astype(BF)
        dg_ref[8 * idx:8 * idx + 8, :] = total

    d_norm = nt(d01_s[rows, :], w_ref[:, C_I0:C_I0 + 2 * FF])
    norm_back(d_norm, lambda off: x2_s[off:off + CHUNK, :], dy_ref, lambda off: dm2_s.at[chunk_rows(off), :], 2)

    tail(0)

    dctx_s[...] = nn(dm2_s[rows, :], w_ref[:, C_CO:C_CO + INNER]).astype(BF)

    def cross_pair_back(hp, carry):
        o = pl.multiple_of(hp * QB, QB)
        cross_masks(o)
        for head in range(2):
            for qb in range(3):
                cols = slice(qb * QB, (qb + 1) * QB)
                d_p = nt(vm_s[head * ENC:(head + 1) * ENC, :], dctx_s[cols, pl.ds(o, QB)]).astype(BF).astype(F32)
                probs = cpf_s[2 * hp + head, :, cols]
                d_l = probs * (d_p - jnp.sum(probs * d_p, axis=0, keepdims=True))
                cds_s[head * ENC:(head + 1) * ENC, cols] = d_l.astype(BF)
        dcq_s[rows, pl.ds(o, QB)] = tn(cds_s[...], km_s[0:2 * ENC, :]).astype(BF)
        d_k = nn(cds_s[...], cq_s[:, pl.ds(o, QB)])
        d_v = nn(cpt_s[hp], dctx_s[:, pl.ds(o, QB)])
        low = lane_idx[:ENC] < 64
        dckv_s[erows, pl.ds(o, QB)] = jnp.where(low, d_k[:ENC], d_k[ENC:]).astype(BF)
        dckv_s[erows, pl.ds(pl.multiple_of(INNER + o, QB), QB)] = jnp.where(low, d_v[:ENC], d_v[ENC:]).astype(BF)
        return carry

    lax.fori_loop(0, PAIRS, cross_pair_back, 0)
    d_norm = nt(dcq_s[rows, :], w_ref[:, C_CQ:C_CQ + INNER])
    wait_slot(2)
    de_buf[slot] = nt(dckv_s[erows, :], w_ref[:, C_CK:C_CK + 2 * INNER]).astype(BF)
    send(2)
    norm_back(d_norm, lambda off: x1_s[off:off + CHUNK, :], dm2_s, lambda off: dm1_s.at[chunk_rows(off), :], 1)

    tail(1)

    dctx_s[...] = nn(dm1_s[rows, :], w_ref[:, C_SO:C_SO + INNER]).astype(BF)

    def self_pair_back(hp, carry):
        o = pl.multiple_of(hp * QB, QB)
        k_pair = qkv_s[:, pl.ds(pl.multiple_of(INNER + o, QB), QB)]
        v_pair = qkv_s[:, pl.ds(pl.multiple_of(2 * INNER + o, QB), QB)]
        for head in range(2):
            km_s[head * SEQ:(head + 1) * SEQ, :] = head_mask(k_pair, head, lane_idx)
            vm_s[head * SEQ:(head + 1) * SEQ, :] = head_mask(v_pair, head, lane_idx)
        for head in range(2):
            for qb in range(3):
                n = QB * (qb + 1)
                cols = slice(qb * QB, (qb + 1) * QB)
                d_p = nt(vm_s[head * SEQ:head * SEQ + n, :], dctx_s[cols, pl.ds(o, QB)]).astype(BF).astype(F32)
                probs = pf_s[2 * hp + head, 0:n, cols]
                d_l = probs * (d_p - jnp.sum(probs * d_p, axis=0, keepdims=True))
                db_ref[2 * hp + head, SEQ - n:SEQ, :] += d_l
                ds_s[head * SEQ:head * SEQ + n, cols] = d_l.astype(BF)
        dqkv_s[rows, pl.ds(o, QB)] = tn(ds_s[...], km_s[...]).astype(BF)
        d_k = nn(ds_s[...], qkv_s[:, pl.ds(o, QB)])
        d_v = nn(pt_s[hp], dctx_s[:, pl.ds(o, QB)])
        low = lane_idx < 64
        dqkv_s[rows, pl.ds(pl.multiple_of(INNER + o, QB), QB)] = jnp.where(low, d_k[:SEQ], d_k[SEQ:]).astype(BF)
        dqkv_s[rows, pl.ds(pl.multiple_of(2 * INNER + o, QB), QB)] = jnp.where(low, d_v[:SEQ], d_v[SEQ:]).astype(BF)
        return carry

    lax.fori_loop(0, PAIRS, self_pair_back, 0)
    d_norm = nt(dqkv_s[rows, :], w_ref[:, C_SQ:C_SQ + 3 * INNER])
    wait_slot(1)
    norm_back(d_norm, lambda off: x_ref[chunk_rows(off), :], dm1_s, lambda off: dx_buf.at[slot, off:off + CHUNK, :], 0)
    send(1)


SCRATCH = [
    ((2 * SEQ, DIM), BF),
    ((2 * SEQ, DIM), BF),
    ((2 * SEQ, DIM), BF),
    ((2 * SEQ, DIM), BF),
    ((2 * SEQ, DIM), BF),
    ((SEQ, 3 * INNER), BF),
    ((2 * SEQ, 3 * INNER), BF),
    ((2 * SEQ, INNER), BF),
    ((SEQ, INNER), BF),
    ((ENC, 2 * INNER), BF),
    ((2 * SEQ, INNER), BF),
    ((2 * ENC, 2 * INNER), BF),
    ((2 * SEQ, INNER), BF),
    ((2 * SEQ, FF), BF),
    ((2 * SEQ, 2 * FF), BF),
    ((SEQ, DIM), BF),
    ((SEQ, DIM), BF),
    ((SEQ, INNER), BF),
    ((HEADS, SEQ, SEQ), F32),
    ((PAIRS, 2 * SEQ, SEQ), BF),
    ((HEADS, ENC, SEQ), F32),
    ((PAIRS, 2 * ENC, SEQ), BF),
    ((2 * SEQ, SEQ), BF),
    ((2 * ENC, SEQ), BF),
    ((2 * SEQ, QB), BF),
    ((2 * SEQ, QB), BF),
]


def add_grad(g_ref, act, d_out, col, width):
    size = 384 if width % 384 == 0 else 512
    for off in range(0, width, size):
        g_ref[:, col + off:col + off + size] += tn(act[...], d_out[:, off:off + size])


def mlp_grads(gm_s, dy_ref, n3_s, hid_s, d01_s):
    add_grad(gm_s, n3_s, d01_s, 0, 2 * FF)
    add_grad(gm_s, dy_ref, hid_s, 2 * FF, FF)


def attn_grads(g_ref, e_ref, n1_s, n2_s, dm1_s, dm2_s, dqkv_s, ctx_s, dcq_s, dckv_s, cctx_s):
    add_grad(g_ref, dm2_s, cctx_s, C_CO, INNER)
    add_grad(g_ref, n2_s, dcq_s, C_CQ, INNER)
    add_grad(g_ref, e_ref, dckv_s, C_CK, 2 * INNER)
    add_grad(g_ref, dm1_s, ctx_s, C_SO, INNER)
    add_grad(g_ref, n1_s, dqkv_s, C_SQ, 3 * INNER)


O_I0, O_I1, O_WO, O_EX, O_END = 2048, 2560, 3072, 3584, 3712
PACKED = (((0, 1024), (O_EX, QB)), ((1024, 1024),), ((O_I0, 1536),))
WHOLE = (((0, 1536), (C_END, QB)), ((1536, 1536),), ((C_I0, 3072),))
X_FIRST = (((0, 768),), ((1536, 768),), ((C_I0, 1536),))
Y_FIRST = (((768, 768), (C_END, QB)), ((2304, 768),), ((C_I0 + 1536, 1536),))
GATHER_SEMS = 48
THRESHOLDS = tuple(range(1, 17)) + BUCKET_EDGES


def gather_plan(loc_ref, rz_s, w_s, send_sem, recv_sem):
    m, d = lax.axis_index("model"), lax.axis_index("data")
    core, x, y = lax.rem(d, 2), lax.rem(d // 2, 2), d // 4
    d_core, d_x, d_y = d + 1 - 2 * core, d + 2 - 4 * x, d + 4 - 8 * y
    count = [0]

    def copy(src, dst, peer):
        number = count[0]
        count[0] += 1
        return lambda: pltpu.make_async_remote_copy(src_ref=src, dst_ref=dst, send_sem=send_sem.at[number], recv_sem=recv_sem.at[number],
                                                    device_id=peer, device_id_type=MESH)

    def block(owner, run):
        return w_s.at[pl.ds(pl.multiple_of(owner * 64, 64), 64), run[0]:run[0] + run[1]]

    def blocks(owners, runs, peer):
        return [copy(block(owner, run), block(owner, run), peer) for owner in owners for run in runs]

    plan = []
    for group in range(3):
        z = [copy(loc_ref.at[:, a:a + n], rz_s.at[:, a:a + n], {"model": 1 - m}) for a, n in PACKED[group]]
        second = blocks([d], X_FIRST[group], {"data": d_x}) + blocks([d], Y_FIRST[group], {"data": d_y})
        third = blocks([d, d_x], X_FIRST[group], {"data": d_y}) + blocks([d, d_y], Y_FIRST[group], {"data": d_x})
        mine = [core, core + 2, core + 4, core + 6]
        plan.append((z, second, third, blocks(mine, WHOLE[group], {"data": d_core})))
    return plan


def pack_share(attn, mlp, ext_ref, loc_s):
    m = lax.axis_index("model")
    for b, ref in enumerate(attn):
        left = jnp.concatenate([ref[...].astype(F32), jnp.zeros((64, 64), F32)], axis=1)
        loc_s[:, 256 * b:256 * b + 256] = jnp.where(m == 0, left, pltpu.roll(left, 64, 1)).astype(BF)
    for col, ref in zip((O_I0, O_I1, O_WO), mlp):
        loc_s[:, col:col + 512] = ref[...]
    loc_s[:, O_EX:O_END] = ext_ref[...]


def fill_gains(w_s, gain_s):
    low = lax.broadcasted_iota(jnp.int32, (8, QB), 1) < 64
    for pair in range(4):
        even = w_s[128 * pair:128 * pair + 16, C_END:C_END + QB].astype(F32)[0:8]
        odd = w_s[128 * pair + 64:128 * pair + 80, C_END:C_END + QB].astype(F32)[0:8]
        gain_s[:, QB * pair:QB * pair + QB] = jnp.where(low, even, pltpu.roll(odd, 64, 1))


def small_grads(dg_s, db_s, ext_ref):
    dist = jnp.maximum(SEQ - QB + lax.broadcasted_iota(jnp.int32, (SEQ, QB), 1) - lax.broadcasted_iota(jnp.int32, (SEQ, QB), 0), 0)
    ids = jnp.zeros((SEQ, QB), jnp.int32)
    for edge in THRESHOLDS:
        ids = ids + (dist >= edge).astype(jnp.int32)
    lane = lax.broadcasted_iota(jnp.int32, (NUM_BUCKETS, QB), 1)
    row = lax.broadcasted_iota(jnp.int32, (NUM_BUCKETS, QB), 0)
    bias = jnp.zeros((NUM_BUCKETS, QB), F32)
    for head in range(HEADS):
        def bucket_sum(bucket, sums):
            part = jnp.sum(jnp.where(ids == bucket, db_s[head], 0.0), axis=0, keepdims=True)
            return jnp.where(row == bucket, part, sums)
        sums = lax.fori_loop(0, NUM_BUCKETS, bucket_sum, jnp.zeros((NUM_BUCKETS, QB), F32))
        bias = jnp.where(lane == 64 + head, jnp.sum(sums, axis=1, keepdims=True), bias)
    row8 = lax.broadcasted_iota(jnp.int32, (8, DIM), 0)
    gains = jnp.zeros((8, DIM), F32)
    for idx in range(3):
        gains = jnp.where(row8 == idx, jnp.sum(dg_s[8 * idx:8 * idx + 8, :], axis=0, keepdims=True), gains)
    low = lax.broadcasted_iota(jnp.int32, (8, QB), 1) < 64
    for d in range(8):
        tile = gains[:, QB * (d // 2):QB * (d // 2) + QB]
        if d % 2:
            tile = pltpu.roll(tile, 64, 1)
        ext_ref[64 * d:64 * d + 8, :] = jnp.where(low, tile, bias[0:8])
        ext_ref[64 * d + 8:64 * d + NUM_BUCKETS, :] = bias[8:]
        ext_ref[64 * d + NUM_BUCKETS:64 * d + 64, :] = jnp.zeros((32, QB), F32)


def merge_share(group, loc_ref, rz_s, w_s):
    m, d = lax.axis_index("model"), lax.axis_index("data")
    rows = pl.ds(pl.multiple_of(d * 64, 64), 64)

    def both(a, n):
        here, there = loc_ref[:, a:a + n].astype(F32), rz_s[:, a:a + n].astype(F32)
        return jnp.where(m == 0, here, there), jnp.where(m == 0, there, here)

    if group == 2:
        for a, col in ((O_I0, C_I0), (O_I1, C_I1), (O_WO, C_WO)):
            low, high = both(a, 512)
            w_s[rows, col:col + 512] = low.astype(BF)
            w_s[rows, col + 512:col + 1024] = high.astype(BF)
        return
    for b in range(4 * group, 4 * group + 4):
        low, high = both(256 * b, 256)
        w_s[rows, INNER * b:INNER * b + QB] = low[:, :QB].astype(BF)
        w_s[rows, INNER * b + QB:INNER * b + 2 * QB] = (low[:, QB:] + high[:, :QB]).astype(BF)
        w_s[rows, INNER * b + 2 * QB:INNER * b + 3 * QB] = high[:, QB:].astype(BF)
    if group == 0:
        w_s[rows, C_END:C_END + QB] = loc_ref[:, O_EX:O_END]


def begin(copies):
    for make in copies:
        make().start()


def arrive_all(copies):
    for make in copies:
        make().wait_recv()


def fill_bias(loc_ref, rz_s, bias_s):
    m = lax.axis_index("model")
    here, there = loc_ref[0:NUM_BUCKETS, O_EX:O_END].astype(F32), rz_s[0:NUM_BUCKETS, O_EX:O_END].astype(F32)
    tables = jnp.where(m == 0, here, there), jnp.where(m == 0, there, here)
    dist = SEQ - QB + lax.broadcasted_iota(jnp.int32, (SEQ, QB), 1) - lax.broadcasted_iota(jnp.int32, (SEQ, QB), 0)
    for head in range(HEADS):
        table = tables[head // 3]
        lane = 64 + head % 3
        value = jnp.broadcast_to(table[0:1, lane:lane + 1], (SEQ, QB))
        for bucket, edge in enumerate(THRESHOLDS):
            value = jnp.where(dist >= edge, table[bucket + 1:bucket + 2, lane:lane + 1], value)
        bias_s[head] = value


def layer_kernel(x_ref, e_ref, dy_ref, *refs):
    attn, mlp, (extra_ref, y_hbm, dx_hbm, de_hbm, g_ref, ext_ref, first_hbm, first_ext, mlp_ref), scratch = refs[:8], refs[8:11], refs[11:20], refs[20:]
    *scratch, y_buf, dx_buf, de_buf, w_ref, rz_s, gain_ref, bias_ref, loc_ref, dg_ref, db_ref, local_sem, send_sem, recv_sem, w_send, w_recv, g_send, g_recv, gm_s, mf_s, mx_s, my_s, m_send, m_recv = scratch
    plan = gather_plan(loc_ref, rz_s, w_ref, w_send, w_recv)
    (n1_s, n2_s, n3_s, dm1_s, dm2_s, qkv_s, dqkv_s, ctx_s, cq_s, ckv_s, dcq_s, dckv_s, cctx_s,
     hid_s, d01_s, x1_s, x2_s, dctx_s, pf_s, pt_s, cpf_s, cpt_s, ds_s, cds_s, km_s, vm_s) = scratch
    me = lax.axis_index("model")
    other = 1 - me
    step = pl.program_id(0)
    seqs = SEQS_STEP * pl.num_programs(0)
    bufs = ((y_buf, y_hbm, SEQ), (dx_buf, dx_hbm, SEQ), (de_buf, de_hbm, ENC))

    @pl.when(step == 0)
    def _():
        d = lax.axis_index("data")
        core, x, y = lax.rem(d, 2), lax.rem(d // 2, 2), d // 4
        barrier = pltpu.get_barrier_semaphore()
        for peer in ({"model": other}, {"data": d + 1 - 2 * core}, {"data": d + 2 - 4 * x}, {"data": d + 4 - 8 * y}):
            pl.semaphore_signal(barrier, inc=1, device_id=peer, device_id_type=MESH)
        pl.semaphore_wait(barrier, 4)
        pack_share(attn, mlp, extra_ref, loc_ref)
        for group in range(3):
            begin(plan[group][0])
        arrive_all(plan[0][0])
        merge_share(0, loc_ref, rz_s, w_ref)
        begin(plan[0][1])
        arrive_all(plan[1][0])
        merge_share(1, loc_ref, rz_s, w_ref)
        begin(plan[1][1])
        arrive_all(plan[0][1])
        begin(plan[0][2])
        arrive_all(plan[2][0])
        merge_share(2, loc_ref, rz_s, w_ref)
        begin(plan[2][1])
        arrive_all(plan[1][1])
        begin(plan[1][2])
        fill_bias(loc_ref, rz_s, bias_ref)
        pt_s[...] = jnp.zeros_like(pt_s)
        ds_s[...] = jnp.zeros_like(ds_s)
        dg_ref[...] = jnp.zeros_like(dg_ref)
        db_ref[...] = jnp.zeros_like(db_ref)
        arrive_all(plan[0][2])
        begin(plan[0][3])
        arrive_all(plan[2][1])
        begin(plan[2][2])
        g_ref[...] = jnp.zeros_like(g_ref)
        gm_s[...] = jnp.zeros_like(gm_s)
        arrive_all(plan[0][3])
        fill_gains(w_ref, gain_ref)

    def copies(which, number):
        buf, hbm, length = bufs[which]
        slot = lax.rem(number, 2)
        rows = pl.ds(pl.multiple_of((me * seqs + number) * length, length), length)
        local = pltpu.make_async_copy(buf.at[slot], hbm.at[rows, :], local_sem.at[which, slot])
        remote = pltpu.make_async_remote_copy(
            src_ref=buf.at[slot], dst_ref=hbm.at[rows, :], send_sem=send_sem.at[which, slot],
            recv_sem=recv_sem.at[which, number], device_id={"model": other}, device_id_type=MESH)
        return local, remote

    d = lax.axis_index("data")
    core, x, y = lax.rem(d, 2), lax.rem(d // 2, 2), d // 4
    to_core, to_x, to_y = {"data": d + 1 - 2 * core}, {"data": d + 2 - 4 * x}, {"data": d + 4 - 8 * y}
    half = (C_END - C_I0) // 2

    def rows_of(yy, xx, cc):
        return pl.ds(pl.multiple_of(64 * (4 * yy + 2 * xx + cc), 64), 64)

    def mlp_copy(number, src, dst, peer):
        return pltpu.make_async_remote_copy(src_ref=src, dst_ref=dst, send_sem=m_send.at[number], recv_sem=m_recv.at[number],
                                            device_id=peer, device_id_type=MESH)

    def mlp_phase(phase):
        if phase == 0:
            return [mlp_copy(b, gm_s.at[rows_of(b // 2, b % 2, 1 - core), :], mf_s.at[64 * b:64 * b + 64, :], to_core) for b in range(4)]
        if phase == 1:
            return ([mlp_copy(4 + b, gm_s.at[rows_of(b, 1 - x, core), 0:half], mx_s.at[64 * b:64 * b + 64, :], to_x) for b in range(2)]
                    + [mlp_copy(6 + b, gm_s.at[rows_of(1 - y, b, core), half:2 * half], my_s.at[64 * b:64 * b + 64, :], to_y) for b in range(2)])
        return []

    def body(s, carry):
        number = step * SEQS_STEP + s

        def tail(point):
            if point == 0:
                @pl.when(s == SEQS_STEP - 1)
                def _():
                    mlp_grads(gm_s, dy_ref, n3_s, hid_s, d01_s)

            @pl.when(number == seqs - 1)
            def _():
                if point == 1:
                    for copy in mlp_phase(0):
                        copy.wait_recv()
                    for b in range(4):
                        gm_s[rows_of(b // 2, b % 2, core), :] += mf_s[64 * b:64 * b + 64, :]
                for copy in mlp_phase(point):
                    copy.start()

        def wait_slot(which):
            @pl.when(number >= 2)
            def _():
                local, remote = copies(which, number - 2)
                local.wait()
                remote.wait_send()

        def send(which):
            local, remote = copies(which, number)
            remote.start()
            local.start()

        def weights_here(group):
            @pl.when(number == 0)
            def _():
                arrive_all(plan[group][2])
                begin(plan[group][3])
                arrive_all(plan[group][3])
                if group == 2:
                    for phases in plan:
                        for phase in phases:
                            for make in phase:
                                make().wait_send()

        seq_body(s, (lax.rem(number, 2), wait_slot, send, weights_here, tail), x_ref, e_ref, dy_ref, w_ref, gain_ref, bias_ref, y_buf, dx_buf, de_buf, dg_ref, db_ref, *scratch)
        return carry

    lax.fori_loop(0, SEQS_STEP, body, 0)
    attn_grads(g_ref, e_ref, n1_s, n2_s, dm1_s, dm2_s, dqkv_s, ctx_s, dcq_s, dckv_s, cctx_s)

    @pl.when(step == pl.num_programs(0) - 1)
    def _():
        def push_core(src, dst, b, number):
            copy = pltpu.make_async_remote_copy(
                src_ref=src.at[rows_of(b // 2, b % 2, 1 - core), :], dst_ref=dst.at[64 * b:64 * b + 64, :],
                send_sem=g_send.at[number], recv_sem=g_recv.at[number], device_id=to_core, device_id_type=MESH)
            copy.start()
            return copy

        pushed = [push_core(g_ref, first_hbm, b, b) for b in range(4)]
        small_grads(dg_ref, db_ref, ext_ref)
        pushed += [push_core(ext_ref, first_ext, b, 4 + b) for b in range(4)]
        for copy in mlp_phase(1):
            copy.wait_recv()
        for b in range(2):
            blk = slice(64 * b, 64 * b + 64)
            mlp_ref[blk, 0:half] = gm_s[rows_of(b, x, core), 0:half] + mx_s[blk, :]
            mlp_ref[blk, half:2 * half] = gm_s[rows_of(y, b, core), half:2 * half] + my_s[blk, :]
        for phase in range(2):
            for copy in mlp_phase(phase):
                copy.wait_send()
        for copy in pushed:
            copy.wait()
        for which in range(3):
            for back in (2, 1):
                local, remote = copies(which, seqs - back)
                local.wait()
                remote.wait_send()

            def arrived(number, carry):
                copies(which, number)[1].wait_recv()
                return carry

            lax.fori_loop(0, seqs, arrived, 0)


R_EX, R_END = C_I0, C_I0 + QB
RUNS = (((0, 1152), (R_EX, QB)), ((1152, 1152),), ((2304, 768),))
MLP_PIECES = ((0, 512, O_I0), (1024, 512, O_I1), (2048, 512, O_WO))


def z_pieces(group):
    attn = [(INNER * b, QB, 256, 256 * b) for b in range(8)]
    if group == 0:
        return attn[:3] + [(R_EX, 0, QB, O_EX)]
    return attn[3:6] if group == 1 else attn[6:]


Z_WIDTH = tuple(sum(piece[2] for piece in z_pieces(group)) for group in range(3))
RUN_WIDTH = tuple(sum(run[1] for run in RUNS[group]) for group in range(3))
REDUCE_SCRATCH = [(2, 2, 64, R_END), (2, 2, 64, R_END),
                  (2, 64, RUN_WIDTH[0]), (64, RUN_WIDTH[0]), (64, Z_WIDTH[0]),
                  (2, 64, RUN_WIDTH[1]), (2, 64, Z_WIDTH[1]), (64, Z_WIDTH[1]),
                  (2, 2, 64, Z_WIDTH[2]), (2, 64, Z_WIDTH[2]), (64, Z_WIDTH[2]), (128, 3072), (64, 3072), (64, 3072), (64, 1536)]
REDUCE_SEMS = 64


def reduce_kernel(g_hbm, ext_hbm, first_hbm, first_ext, mlp_hbm, out_ref, acc, first, a1, a2, a3, b1, b2, b3, c1, c2, c3, mlp_in, mlp_second, mlp_own, mlp_far, local_sem, send_sem, recv_sem):
    m, d = lax.axis_index("model"), lax.axis_index("data")
    core, x, y = lax.rem(d, 2), lax.rem(d // 2, 2), d // 4
    to_x, to_y, to_z = {"data": d + 2 - 4 * x}, {"data": d + 4 - 8 * y}, {"model": 1 - m}
    barrier = pltpu.get_barrier_semaphore()
    for peer in (to_x, to_y, to_z):
        pl.semaphore_signal(barrier, inc=1, device_id=peer, device_id_type=MESH)
    sent = []

    def push(src, dst, peer):
        number = len(sent)
        copy = pltpu.make_async_remote_copy(src_ref=src, dst_ref=dst, send_sem=send_sem.at[number], recv_sem=recv_sem.at[number],
                                            device_id=peer, device_id_type=MESH)
        copy.start()
        sent.append(copy)
        return copy

    def cols(piece, who):
        return pl.ds(pl.multiple_of(piece[0] + who * piece[1], QB), piece[2])

    loads, pend = {}, {}
    number = 0
    for group in (2, 0, 1):
        loads[group] = []
        for col, width in RUNS[group]:
            own, far = (ext_hbm, first_ext) if col == R_EX else (g_hbm, first_hbm)
            src_cols = pl.ds(0 if col == R_EX else col, width)
            for src, dst in ((own.at[:, :, core, :, src_cols], acc), (far.at[:, :, :, src_cols], first)):
                here = pltpu.make_async_copy(src, dst.at[:, :, :, pl.ds(col, width)], local_sem.at[number])
                number += 1
                here.start()
                loads[group].append(here)
    mlp_load = pltpu.make_async_copy(mlp_hbm, mlp_in, local_sem.at[number])
    mlp_load.start()
    pl.semaphore_wait(barrier, 3)
    mlp_load.wait()
    def rows64(blk):
        return pl.ds(pl.multiple_of(64 * blk, 64), 64)

    mlp_pend = [push(mlp_in.at[rows64(1 - y), 0:1536], mlp_second.at[:, 0:1536], to_y),
                push(mlp_in.at[rows64(1 - x), 1536:3072], mlp_second.at[:, 1536:3072], to_x)]

    def run_push(group, src_of, dst, peer):
        off, out = 0, []
        for col, width in RUNS[group]:
            out.append(push(src_of(pl.ds(col, width)), dst.at[..., pl.ds(off, width)], peer))
            off += width
        return out

    def z_push(group, src_of, dst, peer, who):
        off, out = 0, []
        for piece in z_pieces(group):
            out.append(push(src_of(cols(piece, who)), dst.at[..., pl.ds(off, piece[2])], peer))
            off += piece[2]
        return out

    for group in (2, 0, 1):
        for here in loads[group]:
            here.wait()
        for col, width in RUNS[group]:
            for yy in range(2):
                for xx in range(2):
                    acc[yy, xx, :, col:col + width] += first[yy, xx, :, col:col + width]
        if group == 0:
            pend[0] = run_push(0, lambda c: acc.at[:, 1 - x, :, c], a1, to_x)
        elif group == 1:
            pend[1] = run_push(1, lambda c: acc.at[1 - y, :, :, c], b1, to_y)
        else:
            pend[2] = z_push(2, lambda c: acc.at[:, :, :, c], c1, to_z, 1 - m)

    for copy in mlp_pend:
        copy.wait_recv()
    mlp_own[:, 0:1536] = mlp_in[rows64(y), 0:1536] + mlp_second[:, 0:1536]
    mlp_own[:, 1536:3072] = mlp_in[rows64(x), 1536:3072] + mlp_second[:, 1536:3072]
    mlp_pend = [push(mlp_own.at[:, pl.ds(pl.multiple_of(col + (1 - m) * width, QB), width)], mlp_far.at[:, width * n:width * n + width], to_z)
                for n, (col, width, _) in enumerate(MLP_PIECES)]

    def arrive(group):
        for copy in pend[group]:
            copy.wait_recv()

    arrive(0)
    off = 0
    for col, width in RUNS[0]:
        for yy in range(2):
            acc[yy, x, :, col:col + width] += a1[yy, :, off:off + width]
        off += width
    pend[0] = run_push(0, lambda c: acc.at[1 - y, x, :, c], a2, to_y)
    arrive(1)
    off = 0
    for col, width in RUNS[1]:
        for xx in range(2):
            acc[y, xx, :, col:col + width] += b1[xx, :, off:off + width]
        off += width
    pend[1] = z_push(1, lambda c: acc.at[y, :, :, c], b2, to_z, 1 - m)
    held_z = pend[2]
    for copy in held_z:
        copy.wait_recv()
        copy.wait_send()
    off = 0
    for piece in z_pieces(2):
        for yy in range(2):
            for xx in range(2):
                acc[yy, xx, :, cols(piece, m)] += c1[yy, xx, :, off:off + piece[2]]
        off += piece[2]
    pend[2] = z_push(2, lambda c: acc.at[:, 1 - x, :, c], c2, to_x, m)

    arrive(0)
    off = 0
    for col, width in RUNS[0]:
        acc[y, x, :, col:col + width] += a2[:, off:off + width]
        off += width
    pend[0] = z_push(0, lambda c: acc.at[y, x, :, c], a3, to_z, 1 - m)
    held = pend[1]
    for copy in held:
        copy.wait_recv()
        copy.wait_send()
    off = 0
    for piece in z_pieces(1):
        for xx in range(2):
            acc[y, xx, :, cols(piece, m)] += b2[xx, :, off:off + piece[2]]
        off += piece[2]
    pend[1] = z_push(1, lambda c: acc.at[y, 1 - x, :, c], b3, to_x, m)
    arrive(2)
    off = 0
    for piece in z_pieces(2):
        for yy in range(2):
            acc[yy, x, :, cols(piece, m)] += c2[yy, :, off:off + piece[2]]
        off += piece[2]
    pend[2] = z_push(2, lambda c: acc.at[1 - y, x, :, c], c3, to_y, m)

    for group, last in ((0, a3), (1, b3), (2, c3)):
        arrive(group)
        off = 0
        for piece in z_pieces(group):
            out_ref[:, piece[3]:piece[3] + piece[2]] = acc[y, x, :, cols(piece, m)] + last[:, off:off + piece[2]]
            off += piece[2]
    for n, (col, width, place) in enumerate(MLP_PIECES):
        mlp_pend[n].wait_recv()
        mine = pl.ds(pl.multiple_of(col + m * width, QB), width)
        out_ref[:, place:place + width] = mlp_own[:, mine] + mlp_far[:, width * n:width * n + width]
    for copy in sent:
        if not any(copy is other for other in held + held_z):
            copy.wait_send()


def scatter_grads(grad_attn, ext, first, first_ext, mlp):
    m = lax.axis_index("model")
    mine = pl.pallas_call(
        reduce_kernel,
        out_shape=jax.ShapeDtypeStruct((64, O_END), F32),
        in_specs=[pl.BlockSpec(memory_space=pl.ANY)] * 5,
        out_specs=pl.BlockSpec(memory_space=pltpu.VMEM),
        scratch_shapes=[pltpu.VMEM(item, F32) for item in REDUCE_SCRATCH] + [
            pltpu.SemaphoreType.DMA((16,)), pltpu.SemaphoreType.DMA((REDUCE_SEMS,)), pltpu.SemaphoreType.DMA((REDUCE_SEMS,))],
        compiler_params=pltpu.CompilerParams(vmem_limit_bytes=67043328, collective_id=1, has_side_effects=True),
        name="reduce",
    )(grad_attn.reshape(2, 2, 2, 64, C_I0), ext.reshape(2, 2, 2, 64, QB), first.reshape(2, 2, 64, C_I0), first_ext.reshape(2, 2, 64, QB), mlp)
    outs = [jnp.where(m == 0, mine[:, 256 * b:256 * b + 192], mine[:, 256 * b + 64:256 * b + 256]) for b in range(8)]
    outs += [mine[:, O_I0:O_I1], mine[:, O_I1:O_WO], mine[:, O_WO:O_EX]]
    bias = jnp.where(m == 0, mine[:NUM_BUCKETS, O_EX + 64:O_EX + 67], mine[:NUM_BUCKETS, O_EX + 67:O_EX + 70])
    return outs, mine[0:3, O_EX:O_EX + 64], bias


def layer_call(x, e, dy, attn, mlp, extra):
    steps = x.shape[0] // (2 * SEQS_STEP * SEQ)
    part = lambda rows: pl.BlockSpec((rows, DIM), lambda i: (lax.axis_index("model") * steps + i, 0))
    fixed = lambda arr_shape: pl.BlockSpec(arr_shape, lambda i: (0,) * len(arr_shape), pipeline_mode=pl.Buffered(1))
    anywhere = pl.BlockSpec(memory_space=pl.ANY)
    rows, erows = SEQS_STEP * SEQ, SEQS_STEP * ENC
    seqs = SEQS_STEP * steps
    outs = [jax.ShapeDtypeStruct(x.shape, BF), jax.ShapeDtypeStruct(x.shape, BF), jax.ShapeDtypeStruct(e.shape, BF),
            jax.ShapeDtypeStruct((DIM, C_I0), F32), jax.ShapeDtypeStruct((DIM, QB), F32),
            jax.ShapeDtypeStruct((DIM // 2, C_I0), F32), jax.ShapeDtypeStruct((DIM // 2, QB), F32),
            jax.ShapeDtypeStruct((128, C_END - C_I0), F32)]
    return pl.pallas_call(
        layer_kernel,
        out_shape=outs,
        grid=(steps,),
        in_specs=[part(rows), part(erows), part(rows)] + [fixed(w.shape) for w in attn + mlp + [extra]],
        out_specs=[anywhere, anywhere, anywhere, fixed((DIM, C_I0)), fixed((DIM, QB)), anywhere, anywhere, fixed((128, C_END - C_I0))],
        scratch_shapes=[pltpu.VMEM(*item) for item in SCRATCH] + [
            pltpu.VMEM((2, SEQ, DIM), BF), pltpu.VMEM((2, SEQ, DIM), BF), pltpu.VMEM((2, ENC, DIM), BF),
            pltpu.VMEM((DIM, C_END + QB), BF), pltpu.VMEM((64, O_END), BF), pltpu.VMEM((8, DIM), F32), pltpu.VMEM((HEADS, SEQ, QB), F32),
            pltpu.VMEM((64, O_END), BF), pltpu.VMEM((24, DIM), F32), pltpu.VMEM((HEADS, SEQ, QB), F32),
            pltpu.SemaphoreType.DMA((3, 2)), pltpu.SemaphoreType.DMA((3, 2)), pltpu.SemaphoreType.DMA((3, seqs)),
            pltpu.SemaphoreType.DMA((GATHER_SEMS,)), pltpu.SemaphoreType.DMA((GATHER_SEMS,)), pltpu.SemaphoreType.DMA((8,)), pltpu.SemaphoreType.DMA((8,)),
            pltpu.VMEM((DIM, C_END - C_I0), F32), pltpu.VMEM((256, C_END - C_I0), F32), pltpu.VMEM((128, 1536), F32), pltpu.VMEM((128, 1536), F32),
            pltpu.SemaphoreType.DMA((8,)), pltpu.SemaphoreType.DMA((8,))],
        compiler_params=pltpu.CompilerParams(dimension_semantics=("arbitrary",), vmem_limit_bytes=67043328, collective_id=0, has_side_effects=True),
        name="layer",
    )(x, e, dy, *attn, *mlp, extra)


def layer_shard(dec_in, enc_out, grad_out, rel_bias, self_q, self_k, self_v, self_o, cross_q, cross_k, cross_v, cross_o, mlp_wi_0, mlp_wi_1, mlp_wo, norm_self, norm_cross, norm_mlp):
    gains = jnp.stack([norm_self, norm_cross, norm_mlp])
    extra = jnp.pad(gains, ((0, 61), (0, 64))) + jnp.pad(rel_bias, ((0, 32), (64, 61)))

    def flat(arr):
        return arr.reshape(-1, DIM)

    attn = [self_q, self_k, self_v, self_o.T, cross_q, cross_k, cross_v, cross_o.T]
    dec_out, grad_dec, grad_enc, *partial = layer_call(flat(dec_in), flat(enc_out), flat(grad_out), attn, [mlp_wi_0, mlp_wi_1, mlp_wo.T], extra)
    grads, d_gains, grad_bias = scatter_grads(*partial)
    o_sq, o_sk, o_sv, o_so, o_cq, o_ck, o_cv, o_co, o_i0, o_i1, o_wo = grads
    return (dec_out.reshape(dec_in.shape), grad_dec.reshape(dec_in.shape), grad_enc.reshape(enc_out.shape), grad_bias, o_sq, o_sk, o_sv, o_so.T, o_cq, o_ck, o_cv, o_co.T, o_i0, o_i1, o_wo.T, d_gains[0], d_gains[1], d_gains[2])


def solution(mesh):
    row_spec = P("data", None, None)
    col_in = P("data", "model")
    col_out = P("model", "data")
    gain_spec = P("data")
    bias_spec = P(None, "model")
    arg_specs = (row_spec, row_spec, row_spec, bias_spec, col_in, col_in, col_in, col_out, col_in, col_in, col_in, col_out, col_in, col_in, col_out, gain_spec, gain_spec, gain_spec)
    out_specs = (row_spec, row_spec, row_spec) + arg_specs[3:]
    return jax.shard_map(layer_shard, mesh=mesh, in_specs=arg_specs, out_specs=out_specs, check_vma=False)
```
